256 devices in a mesh: rows: 64 (over x, z, y_hi), cols: 4 (over y_lo, core).
Axes of the slice: x: 4, y: 4 (y_hi: 2, y_lo: 2; y = y_hi * 2 + y_lo), z: 8, core: 2. Of those that a mesh axis runs over, the one named last changes fastest.
Arguments:
- matrix: float32 [4096, 32, 2, 128], P('rows', 'cols'), may hold values from -54 to 54
- plan: int32 [2, 4, 256], replicated, may hold values from 0 to 255, as said below
Outputs:
- rotated: float32 [4096, 32, 2, 128], P('rows', 'cols')
The draws below stay inside these ranges and needn't reach their ends.
Inputs may be any that keep to these rules, and one draw needn't show every extreme that they name: Each plan[s, r] pairs the 256 columns: partner of partner of i is i, and no column is its own partner.
All inputs are finite; a program needn't handle non-finite values.
Results may differ from the reference program's by a relative error of at most 0.0003.
Values sent between devices are 32-bit elements; how exact they have to be, the bound alone decides.
No kernel may reach another device: no remote copies, remote signals or barrier semaphores. Data moves between devices by JAX's collectives and lax.ppermute only.
A program may use at most 128 MiB of HBM per device.

```python
import math
import jax
import jax.numpy as jnp
from jax import lax

BLOCK = 128
PAIR_DEV = 8
STEPS = 2
ROUNDS = 4
PAIRS = 32
ROWS = 4096


def draw_matrix(key, part):
    base_key = jax.random.fold_in(key, 11)
    first, second, third = jax.random.split(base_key, 3)
    shape = (ROWS, PAIRS, 2, BLOCK)
    row_scale = jnp.exp(jax.random.uniform(second, (ROWS, 1, 1, 1), jnp.float32, math.log(0.3), math.log(3.0)))
    col_scale = jnp.exp(jax.random.uniform(third, (1, PAIRS, 2, BLOCK), jnp.float32, math.log(0.3), math.log(3.0)))
    values = jnp.clip(jax.random.normal(first, shape, jnp.float32), -6.0, 6.0)
    return (values * row_scale * col_scale).astype(jnp.float32)


def draw_plan(key, part):
    width = 2 * BLOCK

    def one_table(inner_key):
        order = jax.random.permutation(inner_key, width).astype(jnp.int32)
        first_half = order[0::2]
        second_half = order[1::2]
        partner = jnp.zeros((width,), jnp.int32).at[first_half].set(second_half).at[second_half].set(first_half)
        return partner
    keys = jax.random.split(jax.random.fold_in(key, 7), STEPS * ROUNDS)
    tables = jax.vmap(one_table)(keys)
    return tables.reshape(STEPS, ROUNDS, width).astype(jnp.int32)


def setup_inputs(seed: int = 0) -> dict:
    streams_of = jax.random.split(jax.random.key(seed), 3)
    return {
        "matrix": draw_matrix(jax.random.fold_in(streams_of[2], 71), 0),
        "plan": draw_plan(jax.random.fold_in(streams_of[2], 71), 0),
    }


def diagonalize(grams, table):
    width = grams.shape[1]
    indices = jnp.arange(width, dtype=jnp.int32)
    rotation = jnp.broadcast_to(jnp.eye(width, dtype=jnp.float32), grams.shape)
    unit_matrix = jnp.eye(width, dtype=jnp.float32)
    for round_index in range(table.shape[0]):
        partner = table[round_index]
        onehot = (partner[:, None] == indices[None, :]).astype(jnp.float32)
        diagonal_now = jnp.diagonal(grams, axis1=1, axis2=2)
        partner_diag = jnp.einsum('pj,ij->pi', diagonal_now, onehot, precision=lax.Precision.HIGHEST)
        partner_gram = lax.optimization_barrier(jnp.sum(grams * onehot[None], axis=2))
        orient = jnp.where(indices < partner, 1.0, -1.0).astype(jnp.float32)
        spread = orient[None, :] * (partner_diag - diagonal_now)
        sign_part = jnp.where(spread >= 0.0, 1.0, -1.0).astype(jnp.float32)
        tangent = sign_part * 2.0 * partner_gram / (jnp.abs(spread) + jnp.sqrt(spread * spread + 4.0 * partner_gram * partner_gram))
        cosine = 1.0 / jnp.sqrt(1.0 + tangent * tangent)
        sine_part = tangent * cosine
        off_part = jnp.swapaxes(onehot[None] * (-orient[None, :] * sine_part)[:, :, None], 1, 2)
        rot_now = cosine[:, :, None] * unit_matrix[None] + off_part
        product = jnp.einsum('pij,pjk->pik', grams, rot_now, precision=lax.Precision.HIGHEST)
        grams = jnp.einsum('pji,pjk->pik', rot_now, product, precision=lax.Precision.HIGHEST)
        rotation = jnp.einsum('pij,pjk->pik', rotation, rot_now, precision=lax.Precision.HIGHEST)
    return (grams, rotation)

def reference(matrix, plan):
    rows_all, pairs, halves, width = matrix.shape
    columns = matrix.reshape(rows_all, pairs, halves * width)
    for step_index in range(STEPS):
        grams = jnp.einsum('mpi,mpj->pij', columns, columns, precision=lax.Precision.HIGHEST)
        grams, rotation = diagonalize(grams, plan[step_index])
        columns = jnp.einsum('mpi,pij->mpj', columns, rotation, precision=lax.Precision.HIGHEST)
        quarter = columns.reshape(rows_all, pairs, halves, width)
        tops = quarter[:, :, 0, :]
        bottoms = jnp.roll(quarter[:, :, 1, :], PAIR_DEV, axis=1)
        columns = jnp.stack([tops, bottoms], axis=2).reshape(rows_all, pairs, halves * width)
    return columns.reshape(matrix.shape)
```

```python
import functools

import jax
import jax.numpy as jnp
from jax import lax
from jax.experimental import pallas as pl
from jax.experimental.pallas import tpu as pltpu
from jax.sharding import Mesh
from jax.sharding import PartitionSpec as P

STEPS = 2
ROWS = ("x", "z", "yh")
OWNERS = ("x", "yh")
SUMMED = "z"
LINES = 16
CHUNK = 128
F32 = jnp.float32
BF16 = jnp.bfloat16


def one_hot(partner):
    width = partner.shape[1]
    return lax.broadcasted_iota(jnp.int32, (width, width), 0) == partner


def pieces(value):
    high = value.astype(BF16)
    rest = value - high.astype(F32)
    middle = rest.astype(BF16)
    return high, middle, (rest - middle.astype(F32)).astype(BF16)


def permuted(value, table):
    return sum(jnp.dot(part, table, preferred_element_type=F32) for part in pieces(value))


def dot_lines(load, rows, first, second):
    width = first.shape[1]
    table_1 = one_hot(first).astype(BF16)
    table_2 = one_hot(second).astype(BF16)
    total = [jnp.zeros((8, width), F32) for _ in range(10)]
    for start in range(0, rows, CHUNK):
        own = load(start)
        other = permuted(own, table_1)
        own_2 = permuted(own, table_2)
        other_2 = permuted(other, table_2)
        products = (
            own * own,
            other * other,
            own * other,
            own * own_2,
            own * other_2,
            other * own_2,
            other * other_2,
            own_2 * own_2,
            other_2 * other_2,
            own_2 * other_2,
        )
        for i, product in enumerate(products):
            total[i] = total[i] + product.reshape(CHUNK // 8, 8, width).sum(axis=0)
    return [line.sum(axis=0, keepdims=True) for line in total]


def angle(orient, own, other, cross):
    spread = orient * (other - own)
    sign = jnp.where(spread >= 0.0, 1.0, -1.0)
    tangent = sign * 2.0 * cross / (jnp.abs(spread) + jnp.sqrt(spread * spread + 4.0 * cross * cross))
    cosine = 1.0 / jnp.sqrt(1.0 + tangent * tangent)
    return cosine, -orient * (tangent * cosine)


def two_rounds(lines, first, second):
    width = first.shape[1]
    own, other, cross, a, b, c, d, own_2, other_2, cross_2 = (lines[i : i + 1] for i in range(10))
    indices = lax.broadcasted_iota(jnp.int32, (1, width), 1)
    table_2 = one_hot(second)
    wide = jnp.broadcast_to(first.astype(F32).astype(BF16), (16, width))
    far = jnp.dot(wide, table_2.astype(BF16), preferred_element_type=F32)[:1].astype(jnp.int32)
    cos, sin = angle(jnp.where(indices < first, 1.0, -1.0), own, other, cross)
    cos_2, sin_2 = angle(jnp.where(second < far, 1.0, -1.0), own_2, other_2, cross_2)
    diag = cos * cos * own + 2.0 * cos * sin * cross + sin * sin * other
    diag_2 = cos_2 * cos_2 * own_2 + 2.0 * cos_2 * sin_2 * cross_2 + sin_2 * sin_2 * other_2
    joint = cos * cos_2 * a + cos * sin_2 * b + sin * cos_2 * c + sin * sin_2 * d
    cos_b, sin_b = angle(jnp.where(indices < second, 1.0, -1.0), diag, diag_2, joint)
    zero = jnp.zeros((width, width), F32)
    rotation = jnp.where(one_hot(indices), cos_b * cos, zero)
    rotation += jnp.where(one_hot(first), cos_b * sin, zero)
    rotation += jnp.where(table_2, sin_b * cos_2, zero)
    rotation += jnp.where(one_hot(far), sin_b * sin_2, zero)
    return rotation


def write_lines(lines, out_ref):
    lines = lines + [jnp.zeros_like(lines[0])] * (LINES - len(lines))
    block = jnp.concatenate(lines, axis=0)
    for i in range(out_ref.shape[0]):
        out_ref[i] = block


def plan_lines(plan_ref, number):
    return plan_ref[2 * number : 2 * number + 1], plan_ref[2 * number + 1 : 2 * number + 2]


def sort_kernel(in_ref, out_ref):
    rows, owners = out_ref.shape[1], out_ref.shape[0]
    for i in range(owners):
        for half in range(2):
            out_ref[i, :, half * 128 : half * 128 + 128] = in_ref[pl.ds(2 * i + half, rows, 2 * owners), :]


def unsort_kernel(in_ref, out_ref):
    rows, owners = in_ref.shape[1], in_ref.shape[0]
    for i in range(owners):
        for half in range(2):
            out_ref[pl.ds(2 * i + half, rows, 2 * owners), :] = in_ref[i, :, half * 128 : half * 128 + 128]


def first_kernel(number, plan_ref, x_ref, out_ref):
    lines = dot_lines(lambda start: x_ref[start : start + CHUNK], x_ref.shape[0], *plan_lines(plan_ref, number))
    write_lines(lines, out_ref)


def joined_kernel(number, plan_ref, top_ref, bottom_ref, out_ref, x_ref):
    width = top_ref.shape[1]
    x_ref[:, :width] = top_ref[...]
    x_ref[:, width:] = bottom_ref[...]
    lines = dot_lines(lambda start: x_ref[start : start + CHUNK], x_ref.shape[0], *plan_lines(plan_ref, number))
    write_lines(lines, out_ref)


def rotated(number, plan_ref, part_ref, x_ref):
    lines = jnp.sum(part_ref[...], axis=0)
    rotation = two_rounds(lines, *plan_lines(plan_ref, number))
    return jnp.dot(x_ref[...], rotation, precision=lax.Precision.HIGHEST, preferred_element_type=F32)


def middle_kernel(number, plan_ref, part_ref, x_ref, out_ref, y_ref):
    y_ref[...] = rotated(number, plan_ref, part_ref, x_ref)
    lines = dot_lines(lambda start: y_ref[start : start + CHUNK], y_ref.shape[0], *plan_lines(plan_ref, number + 1))
    write_lines(lines, out_ref)


def last_kernel(number, plan_ref, part_ref, x_ref, top_ref, bottom_ref):
    width = top_ref.shape[1]
    result = rotated(number, plan_ref, part_ref, x_ref)
    top_ref[...] = result[:, :width]
    bottom_ref[...] = result[:, width:]


def call(kernel, outs, *args):
    shapes = [jax.ShapeDtypeStruct(shape, F32) for shape in outs]
    single = len(shapes) == 1
    return pl.pallas_call(kernel, out_shape=shapes[0] if single else shapes)(*args)


def exchanged(value, axis):
    return lax.all_to_all(value, axis, split_axis=0, concat_axis=0, tiled=True)


def passed_along(block, axis, distance):
    devices = range(lax.axis_size(axis))
    route = [((i - distance) % len(devices), i) for i in devices]
    return lax.ppermute(block, axis, route)


def body(matrix, plan):
    rows, owners, halves, width = matrix.shape
    peers = lax.axis_size(SUMMED)
    flat = (rows * owners, halves * width)
    half = (rows * owners, width)
    sent = (peers, LINES, halves * width)
    tables = plan.reshape(-1, plan.shape[-1])
    lines = matrix.reshape(rows * owners * halves, width)
    x = exchanged(call(sort_kernel, [(owners, rows, halves * width)], lines), OWNERS).reshape(flat)
    part = call(functools.partial(first_kernel, 0), [sent], tables, x)
    for step in range(STEPS):
        part, x = call(
            functools.partial(middle_kernel, 2 * step), [sent, flat], tables, exchanged(part, SUMMED), x
        )
        top, bottom = call(
            functools.partial(last_kernel, 2 * step + 1), [half, half], tables, exchanged(part, SUMMED), x
        )
        bottom = passed_along(bottom, "cols", 1)
        if step + 1 < STEPS:
            part, x = call(functools.partial(joined_kernel, 2 * step + 2), [sent, flat], tables, top, bottom)
    x = jnp.concatenate([top, bottom], axis=1).reshape(owners, rows, halves * width)
    return call(unsort_kernel, [lines.shape], exchanged(x, OWNERS)).reshape(matrix.shape)


def solution(mesh):
    split = Mesh(mesh.devices.reshape(4, 8, 2, mesh.shape["cols"]), ("x", "z", "yh", "cols"))
    in_specs = (P(ROWS, "cols", None, None), P())
    out_specs = P(ROWS, "cols", None, None)
    return jax.shard_map(body, mesh=split, in_specs=in_specs, out_specs=out_specs, check_vma=False)
```

```python
import functools

import jax
import jax.numpy as jnp
from jax import lax
from jax.experimental import pallas as pl
from jax.experimental.pallas import tpu as pltpu
from jax.sharding import Mesh
from jax.sharding import PartitionSpec as P

STEPS = 2
ROWS = ("x", "z", "yh")
OWNERS = ("x", "yh")
SUMMED = "z"
LINES = 8
CHUNK = 128
VMEM_BYTES = 16 * 1024 * 1024
F32 = jnp.float32
BF16 = jnp.bfloat16


def one_hot(partner):
    width = partner.shape[1]
    return lax.broadcasted_iota(jnp.int32, (width, width), 0) == partner


def pieces(value):
    high = value.astype(BF16)
    rest = value - high.astype(F32)
    middle = rest.astype(BF16)
    return high, middle, (rest - middle.astype(F32)).astype(BF16)


def permuted(value, table):
    return sum(jnp.dot(part, table, preferred_element_type=F32) for part in pieces(value))


def dot_lines(load, rows, first, second, far):
    width = first.shape[1]
    table = jnp.concatenate([one_hot(partner).astype(BF16) for partner in (first, second, far)], axis=1)
    total = [jnp.zeros((8, width), F32) for _ in range(7)]
    for start in range(0, rows, CHUNK):
        own = load(start)
        others = permuted(own, table)
        other, own_2, other_2 = (others[:, i * width : i * width + width] for i in range(3))
        products = (
            own * own,
            other * other,
            own * other,
            own * own_2,
            own * other_2,
            other * own_2,
            other * other_2,
        )
        for i, product in enumerate(products):
            total[i] = total[i] + product.reshape(CHUNK // 8, 8, width).sum(axis=0)
    return [line.sum(axis=0, keepdims=True) for line in total]


def angle(orient, own, other, cross):
    spread = orient * (other - own)
    sign = jnp.where(spread >= 0.0, 1.0, -1.0)
    tangent = sign * 2.0 * cross / (jnp.abs(spread) + jnp.sqrt(spread * spread + 4.0 * cross * cross))
    cosine = 1.0 / jnp.sqrt(1.0 + tangent * tangent)
    return cosine, -orient * (tangent * cosine)


def two_rounds(lines, first, second, far):
    width = first.shape[1]
    table_2 = one_hot(second)
    moved = permuted(lines, table_2.astype(BF16))
    own, other, cross, a, b, c, d = (lines[i : i + 1] for i in range(7))
    own_2, other_2, cross_2 = (moved[i : i + 1] for i in range(3))
    indices = lax.broadcasted_iota(jnp.int32, (1, width), 1)
    cos, sin = angle(jnp.where(indices < first, 1.0, -1.0), own, other, cross)
    cos_2, sin_2 = angle(jnp.where(second < far, 1.0, -1.0), own_2, other_2, cross_2)
    diag = cos * cos * own + 2.0 * cos * sin * cross + sin * sin * other
    diag_2 = cos_2 * cos_2 * own_2 + 2.0 * cos_2 * sin_2 * cross_2 + sin_2 * sin_2 * other_2
    joint = cos * cos_2 * a + cos * sin_2 * b + sin * cos_2 * c + sin * sin_2 * d
    cos_b, sin_b = angle(jnp.where(indices < second, 1.0, -1.0), diag, diag_2, joint)
    zero = jnp.zeros((width, width), F32)
    rotation = jnp.where(one_hot(indices), cos_b * cos, zero)
    rotation += jnp.where(one_hot(first), cos_b * sin, zero)
    rotation += jnp.where(table_2, sin_b * cos_2, zero)
    rotation += jnp.where(one_hot(far), sin_b * sin_2, zero)
    return rotation


def write_lines(lines, out_ref):
    lines = lines + [jnp.zeros_like(lines[0])] * (LINES - len(lines))
    block = jnp.concatenate(lines, axis=0)
    for i in range(out_ref.shape[0]):
        out_ref[i] = block


def plan_lines(plan_ref, number):
    return tuple(plan_ref[number, i : i + 1] for i in range(3))


def plan_kernel(plan_ref, out_ref):
    width = plan_ref.shape[1]
    for i in range(out_ref.shape[0]):
        first, second = plan_ref[2 * i : 2 * i + 1], plan_ref[2 * i + 1 : 2 * i + 2]
        wide = jnp.broadcast_to(first.astype(F32).astype(BF16), (16, width))
        far = jnp.dot(wide, one_hot(second).astype(BF16), preferred_element_type=F32)[:1]
        out_ref[i] = jnp.concatenate([first, second, far.astype(jnp.int32)] + [first] * 5, axis=0)


def sort_kernel(in_ref, out_ref):
    rows, owners = out_ref.shape[1], out_ref.shape[0]
    for i in range(owners):
        for half in range(2):
            out_ref[i, :, half * 128 : half * 128 + 128] = in_ref[pl.ds(2 * i + half, rows, 2 * owners), :]


def unsort_kernel(in_ref, out_ref):
    rows, owners = in_ref.shape[1], in_ref.shape[0]
    for i in range(owners):
        for half in range(2):
            out_ref[pl.ds(2 * i + half, rows, 2 * owners), :] = in_ref[i, :, half * 128 : half * 128 + 128]


def first_kernel(number, plan_ref, x_ref, out_ref):
    lines = dot_lines(lambda start: x_ref[start : start + CHUNK], x_ref.shape[0], *plan_lines(plan_ref, number))
    write_lines(lines, out_ref)


def joined_kernel(number, plan_ref, top_ref, bottom_ref, out_ref, x_ref):
    width = top_ref.shape[1]
    x_ref[:, :width] = top_ref[...]
    x_ref[:, width:] = bottom_ref[...]
    lines = dot_lines(lambda start: x_ref[start : start + CHUNK], x_ref.shape[0], *plan_lines(plan_ref, number))
    write_lines(lines, out_ref)


def rotated(number, plan_ref, part_ref, x_ref):
    lines = jnp.sum(part_ref[...], axis=0)
    rotation = two_rounds(lines, *plan_lines(plan_ref, number))
    return jnp.dot(x_ref[...], rotation, precision=lax.Precision.HIGHEST, preferred_element_type=F32)


def middle_kernel(number, plan_ref, part_ref, x_ref, out_ref, y_ref):
    y_ref[...] = rotated(number, plan_ref, part_ref, x_ref)
    lines = dot_lines(lambda start: y_ref[start : start + CHUNK], y_ref.shape[0], *plan_lines(plan_ref, number + 1))
    write_lines(lines, out_ref)


def last_kernel(number, plan_ref, part_ref, x_ref, top_ref, bottom_ref):
    width = top_ref.shape[1]
    result = rotated(number, plan_ref, part_ref, x_ref)
    top_ref[...] = result[:, :width]
    bottom_ref[...] = result[:, width:]


def call(kernel, outs, *args):
    shapes = [jax.ShapeDtypeStruct(shape, dtype) for shape, dtype in outs]
    single = len(shapes) == 1
    params = pltpu.CompilerParams(vmem_limit_bytes=VMEM_BYTES)
    return pl.pallas_call(kernel, out_shape=shapes[0] if single else shapes, compiler_params=params)(*args)


def exchanged(value, axis):
    return lax.all_to_all(value, axis, split_axis=0, concat_axis=0, tiled=True)


def passed_along(block, axis, distance):
    devices = range(lax.axis_size(axis))
    route = [((i - distance) % len(devices), i) for i in devices]
    return lax.ppermute(block, axis, route)


def body(matrix, plan):
    rows, owners, halves, width = matrix.shape
    peers = lax.axis_size(SUMMED)
    flat = ((rows * owners, halves * width), F32)
    half = ((rows * owners, width), F32)
    sorted_rows = ((owners, rows, halves * width), F32)
    sent = ((peers, LINES, halves * width), F32)
    lines = matrix.reshape(rows * owners * halves, width)
    pairs = plan.reshape(-1, plan.shape[-1])
    x = exchanged(call(sort_kernel, [sorted_rows], lines), OWNERS).reshape(flat[0])
    tables = call(plan_kernel, [((pairs.shape[0] // 2, 8, pairs.shape[1]), jnp.int32)], pairs)
    part = call(functools.partial(first_kernel, 0), [sent], tables, x)
    for step in range(STEPS):
        part, x = call(
            functools.partial(middle_kernel, 2 * step), [sent, flat], tables, exchanged(part, SUMMED), x
        )
        top, bottom = call(
            functools.partial(last_kernel, 2 * step + 1), [half, half], tables, exchanged(part, SUMMED), x
        )
        bottom = passed_along(bottom, "cols", 1)
        if step + 1 < STEPS:
            part, x = call(functools.partial(joined_kernel, 2 * step + 2), [sent, flat], tables, top, bottom)
    x = jnp.concatenate([top, bottom], axis=1).reshape(sorted_rows[0])
    return call(unsort_kernel, [(lines.shape, F32)], exchanged(x, OWNERS)).reshape(matrix.shape)


def solution(mesh):
    split = Mesh(mesh.devices.reshape(4, 8, 2, mesh.shape["cols"]), ("x", "z", "yh", "cols"))
    in_specs = (P(ROWS, "cols", None, None), P())
    out_specs = P(ROWS, "cols", None, None)
    return jax.shard_map(body, mesh=split, in_specs=in_specs, out_specs=out_specs, check_vma=False)
```

```python
import functools

import jax
import jax.numpy as jnp
from jax import lax
from jax.experimental import pallas as pl
from jax.experimental.pallas import tpu as pltpu
from jax.sharding import Mesh
from jax.sharding import PartitionSpec as P

STEPS = 2
ROWS = ("x", "z", "yh")
OWNERS = ("x", "yh")
SUMMED = "z"
LINES = 8
CHUNK = 128
VMEM_BYTES = 16 * 1024 * 1024
F32 = jnp.float32
BF16 = jnp.bfloat16


def one_hot(partner):
    width = partner.shape[1]
    return lax.broadcasted_iota(jnp.int32, (width, width), 0) == partner


def pieces(value):
    high = value.astype(BF16)
    rest = value - high.astype(F32)
    middle = rest.astype(BF16)
    return high, middle, (rest - middle.astype(F32)).astype(BF16)


def permuted(value, table):
    return sum(jnp.dot(part, table, preferred_element_type=F32) for part in pieces(value))


def dot_lines(load, rows, first, second, far):
    width = first.shape[1]
    table = jnp.concatenate([one_hot(partner).astype(BF16) for partner in (first, second, far)], axis=1)
    total = [jnp.zeros((8, width), F32) for _ in range(7)]
    for start in range(0, rows, CHUNK):
        own = load(start)
        others = permuted(own, table)
        other, own_2, other_2 = (others[:, i * width : i * width + width] for i in range(3))
        products = (
            own * own,
            other * other,
            own * other,
            own * own_2,
            own * other_2,
            other * own_2,
            other * other_2,
        )
        for i, product in enumerate(products):
            total[i] = total[i] + product.reshape(CHUNK // 8, 8, width).sum(axis=0)
    return [line.sum(axis=0, keepdims=True) for line in total]


def angle(orient, own, other, cross):
    spread = orient * (other - own)
    sign = jnp.where(spread >= 0.0, 1.0, -1.0)
    tangent = sign * 2.0 * cross / (jnp.abs(spread) + jnp.sqrt(spread * spread + 4.0 * cross * cross))
    cosine = 1.0 / jnp.sqrt(1.0 + tangent * tangent)
    return cosine, -orient * (tangent * cosine)


def two_rounds(lines, first, second, far, columns):
    width = first.shape[1]
    moved = permuted(lines, one_hot(second).astype(BF16))
    own, other, cross, a, b, c, d = (lines[i : i + 1] for i in range(7))
    own_2, other_2, cross_2 = (moved[i : i + 1] for i in range(3))
    indices = lax.broadcasted_iota(jnp.int32, (1, width), 1)
    cos, sin = angle(jnp.where(indices < first, 1.0, -1.0), own, other, cross)
    cos_2, sin_2 = angle(jnp.where(second < far, 1.0, -1.0), own_2, other_2, cross_2)
    diag = cos * cos * own + 2.0 * cos * sin * cross + sin * sin * other
    diag_2 = cos_2 * cos_2 * own_2 + 2.0 * cos_2 * sin_2 * cross_2 + sin_2 * sin_2 * other_2
    joint = cos * cos_2 * a + cos * sin_2 * b + sin * cos_2 * c + sin * sin_2 * d
    cos_b, sin_b = angle(jnp.where(indices < second, 1.0, -1.0), diag, diag_2, joint)
    terms = ((indices, cos_b * cos), (first, cos_b * sin), (second, sin_b * cos_2), (far, sin_b * sin_2))
    line = lax.broadcasted_iota(jnp.int32, (width, columns.stop - columns.start), 0)
    return sum(jnp.where(line == place[:, columns], value[:, columns], 0.0) for place, value in terms)


def write_lines(lines, out_ref):
    lines = lines + [jnp.zeros_like(lines[0])] * (LINES - len(lines))
    block = jnp.concatenate(lines, axis=0)
    for i in range(out_ref.shape[0]):
        out_ref[i] = block


def plan_lines(plan_ref, number):
    return tuple(plan_ref[number, i : i + 1] for i in range(3))


def plan_kernel(plan_ref, out_ref):
    width = plan_ref.shape[1]
    for i in range(out_ref.shape[0]):
        first, second = plan_ref[2 * i : 2 * i + 1], plan_ref[2 * i + 1 : 2 * i + 2]
        wide = jnp.broadcast_to(first.astype(F32).astype(BF16), (16, width))
        far = jnp.dot(wide, one_hot(second).astype(BF16), preferred_element_type=F32)[:1]
        out_ref[i] = jnp.concatenate([first, second, far.astype(jnp.int32)] + [first] * 5, axis=0)


def sort_kernel(in_ref, out_ref):
    rows, owners = out_ref.shape[1], out_ref.shape[0]
    for i in range(owners):
        for half in range(2):
            out_ref[i, :, half * 128 : half * 128 + 128] = in_ref[pl.ds(2 * i + half, rows, 2 * owners), :]


def unsort_kernel(in_ref, out_ref):
    rows, owners = in_ref.shape[1], in_ref.shape[0]
    for i in range(owners):
        for half in range(2):
            out_ref[pl.ds(2 * i + half, rows, 2 * owners), :] = in_ref[i, :, half * 128 : half * 128 + 128]


def first_kernel(number, plan_ref, x_ref, out_ref):
    lines = dot_lines(lambda start: x_ref[start : start + CHUNK], x_ref.shape[0], *plan_lines(plan_ref, number))
    write_lines(lines, out_ref)


def rotated(number, plan_ref, part_ref, x_ref, columns):
    rotation = two_rounds(jnp.sum(part_ref[...], axis=0), *plan_lines(plan_ref, number), columns)
    return jnp.dot(x_ref[...], rotation, precision=lax.Precision.HIGHEST, preferred_element_type=F32)


def middle_kernel(number, plan_ref, part_ref, x_ref, out_ref, y_ref):
    y_ref[...] = rotated(number, plan_ref, part_ref, x_ref, slice(0, x_ref.shape[1]))
    lines = dot_lines(lambda start: y_ref[start : start + CHUNK], y_ref.shape[0], *plan_lines(plan_ref, number + 1))
    write_lines(lines, out_ref)


def top_kernel(number, plan_ref, part_ref, x_ref, top_ref):
    top_ref[...] = rotated(number, plan_ref, part_ref, x_ref, slice(0, top_ref.shape[1]))


def bottom_kernel(number, plan_ref, part_ref, x_ref, top_ref, y_ref):
    width = top_ref.shape[1]
    y_ref[:, :width] = top_ref[...]
    y_ref[:, width:] = rotated(number, plan_ref, part_ref, x_ref, slice(width, 2 * width))


def joined_kernel(number, plan_ref, part_ref, x_ref, top_ref, out_ref, y_ref):
    bottom_kernel(number, plan_ref, part_ref, x_ref, top_ref, y_ref)
    lines = dot_lines(lambda start: y_ref[start : start + CHUNK], y_ref.shape[0], *plan_lines(plan_ref, number + 1))
    write_lines(lines, out_ref)


def call(kernel, outs, *args):
    shapes = [jax.ShapeDtypeStruct(shape, dtype) for shape, dtype in outs]
    single = len(shapes) == 1
    params = pltpu.CompilerParams(vmem_limit_bytes=VMEM_BYTES)
    return pl.pallas_call(kernel, out_shape=shapes[0] if single else shapes, compiler_params=params)(*args)


def exchanged(value, axis):
    return lax.all_to_all(value, axis, split_axis=0, concat_axis=0, tiled=True)


def passed_along(block, axis, distance):
    devices = range(lax.axis_size(axis))
    route = [((i - distance) % len(devices), i) for i in devices]
    return lax.ppermute(block, axis, route)


def body(matrix, plan):
    rows, owners, halves, width = matrix.shape
    peers = lax.axis_size(SUMMED)
    flat = ((rows * owners, halves * width), F32)
    half = ((rows * owners, width), F32)
    sorted_rows = ((owners, rows, halves * width), F32)
    sent = ((peers, LINES, halves * width), F32)
    lines = matrix.reshape(rows * owners * halves, width)
    pairs = plan.reshape(-1, plan.shape[-1])
    x = exchanged(call(sort_kernel, [sorted_rows], lines), OWNERS).reshape(flat[0])
    tables = call(plan_kernel, [((pairs.shape[0] // 2, 8, pairs.shape[1]), jnp.int32)], pairs)
    part = call(functools.partial(first_kernel, 0), [sent], tables, x)
    for step in range(STEPS):
        part, x = call(
            functools.partial(middle_kernel, 2 * step), [sent, flat], tables, exchanged(part, SUMMED), x
        )
        x_before = passed_along(x, "cols", 1)
        part = exchanged(part, SUMMED)
        part_before = passed_along(part, "cols", 1)
        number = 2 * step + 1
        top = call(functools.partial(top_kernel, number), [half], tables, part, x)
        if step + 1 < STEPS:
            part, x = call(
                functools.partial(joined_kernel, number), [sent, flat], tables, part_before, x_before, top
            )
        else:
            x = call(functools.partial(bottom_kernel, number), [flat], tables, part_before, x_before, top)
    x = exchanged(x.reshape(sorted_rows[0]), OWNERS)
    return call(unsort_kernel, [(lines.shape, F32)], x).reshape(matrix.shape)


def solution(mesh):
    split = Mesh(mesh.devices.reshape(4, 8, 2, mesh.shape["cols"]), ("x", "z", "yh", "cols"))
    in_specs = (P(ROWS, "cols", None, None), P())
    out_specs = P(ROWS, "cols", None, None)
    return jax.shard_map(body, mesh=split, in_specs=in_specs, out_specs=out_specs, check_vma=False)
```

```python
import jax
import jax.numpy as jnp
from jax import lax
from jax.experimental import pallas as pl
from jax.experimental.pallas import tpu as pltpu
from jax.sharding import Mesh
from jax.sharding import PartitionSpec as P

STEPS = 2
ROWS = ("x", "z", "yh")
OWNERS = ("x", "yh")
SUMMED = "z"
ROUNDS = 4
WORDS = 1 << ROUNDS
LINES = 56
VMEM_BYTES = 16 * 1024 * 1024
F32 = jnp.float32
BF16 = jnp.bfloat16


def one_hot(partner):
    width = partner.shape[1]
    return lax.broadcasted_iota(jnp.int32, (width, width), 0) == partner


def pieces(value):
    high = value.astype(BF16)
    rest = value - high.astype(F32)
    middle = rest.astype(BF16)
    return high, middle, (rest - middle.astype(F32)).astype(BF16)


def permuted(value, table):
    return sum(jnp.dot(part, table, preferred_element_type=F32) for part in pieces(value))


def angle(orient, own, other, cross):
    spread = orient * (other - own)
    sign = jnp.where(spread >= 0.0, 1.0, -1.0)
    tangent = sign * 2.0 * cross / (jnp.abs(spread) + jnp.sqrt(spread * spread + 4.0 * cross * cross))
    cosine = 1.0 / jnp.sqrt(1.0 + tangent * tangent)
    return cosine, -orient * (tangent * cosine)


def write_lines(x, words_ref, table_ref, out_ref):
    width = x.shape[1]
    gram = lax.dot_general(
        x, x, (((0,), (0,)), ((), ())), precision=lax.Precision.HIGHEST, preferred_element_type=F32
    )
    parts = pieces(gram)
    line = lax.broadcasted_iota(jnp.int32, (width, width), 0)

    def picked(value, word):
        return jnp.where(line == words_ref[word : word + 1], value, 0.0).sum(axis=0, keepdims=True)

    def written(place, value):
        for i in range(out_ref.shape[0]):
            out_ref[i, place : place + 1] = value

    written(0, picked(gram, 0))
    for number in range(ROUNDS):
        count = 1 << number
        for right in range(count):
            column = (count + right - 1) * width
            moved = sum(
                jnp.dot(part, table_ref[:, column : column + width], preferred_element_type=F32) for part in parts
            )
            for left in range(right + 1):
                written(place_of(number, left, right), picked(moved, left))


def place_of(number, left, right):
    return 1 + sum((1 << i) * ((1 << i) + 1) // 2 for i in range(number)) + right * (right + 1) // 2 + left


def table_of(table_ref, number):
    width = table_ref.shape[0]
    column = ((1 << number) - 1) * width
    return table_ref[:, column : column + width]


def angles_kernel(words_ref, table_ref, part_ref, out_ref, lines_ref, moved_ref, state_ref):
    width = words_ref.shape[1]
    lines = jnp.sum(part_ref[...], axis=0)
    lines_ref[...] = lines
    split = pieces(lines)
    for number in range(ROUNDS):
        table = table_of(table_ref, number)
        moved_ref[number] = sum(jnp.dot(part, table, preferred_element_type=F32) for part in split)
    indices = lax.broadcasted_iota(jnp.int32, (1, width), 1)
    state_ref[...] = jnp.zeros_like(state_ref)
    diag, diag_2 = lines_ref[:1], moved_ref[0, :1]
    weights, weights_2 = [jnp.ones((1, width), F32)], [jnp.ones((1, width), F32)]
    for number in range(ROUNDS):
        count = 1 << number
        if number:
            for i, value in enumerate([diag] + weights):
                state_ref[i : i + 1] = value
            other = permuted(state_ref[...], table_of(table_ref, number))
            diag_2, *weights_2 = (other[i : i + 1] for i in range(1 + count))
        cross = jnp.zeros((1, width), F32)
        for left in range(count):
            inner = jnp.zeros((1, width), F32)
            for right in range(count):
                place = place_of(number, min(left, right), max(left, right))
                source = lines_ref[place : place + 1] if left <= right else moved_ref[number, place : place + 1]
                inner += weights_2[right] * source
            cross += weights[left] * inner
        orient = jnp.where(indices < words_ref[count : count + 1], 1.0, -1.0)
        cos, sin = angle(orient, diag, diag_2, cross)
        diag = cos * cos * diag + 2.0 * cos * sin * cross + sin * sin * diag_2
        weights = [cos * value for value in weights] + [sin * value for value in weights_2]
    for i, value in enumerate(weights):
        out_ref[i : i + 1] = value


def plan_kernel(plan_ref, *out_refs):
    width = plan_ref.shape[1]
    steps = len(out_refs) // 2
    for step in range(steps):
        words_ref, table_ref = out_refs[step], out_refs[steps + step]
        words_ref[:1] = lax.broadcasted_iota(jnp.int32, (1, width), 1)
        for number in range(ROUNDS):
            count = 1 << number
            partner = plan_ref[step * ROUNDS + number : step * ROUNDS + number + 1]
            table = one_hot(partner).astype(BF16)
            known = words_ref[...].astype(F32).astype(BF16)
            moved = jnp.dot(known, table, preferred_element_type=F32)
            for i in range(count):
                words_ref[count + i : count + i + 1] = moved[i : i + 1].astype(jnp.int32)
        for word in range(1, WORDS):
            column = (word - 1) * width
            table_ref[:, column : column + width] = one_hot(words_ref[word : word + 1]).astype(BF16)


def sort_kernel(in_ref, out_ref):
    rows, owners = out_ref.shape[1], out_ref.shape[0]
    for i in range(owners):
        for half in range(2):
            out_ref[i, :, half * 128 : half * 128 + 128] = in_ref[pl.ds(2 * i + half, rows, 2 * owners), :]


def unsort_kernel(in_ref, out_ref):
    rows, owners = in_ref.shape[1], in_ref.shape[0]
    for i in range(owners):
        for half in range(2):
            out_ref[pl.ds(2 * i + half, rows, 2 * owners), :] = in_ref[i, :, half * 128 : half * 128 + 128]


def rotated(words_ref, weights_ref, x_ref, columns):
    line = lax.broadcasted_iota(jnp.int32, (x_ref.shape[1], columns.stop - columns.start), 0)
    rotation = jnp.zeros(line.shape, F32)
    for i in range(WORDS):
        rotation += jnp.where(line == words_ref[i : i + 1, columns], weights_ref[i : i + 1, columns], 0.0)
    return jnp.dot(x_ref[...], rotation, precision=lax.Precision.HIGHEST, preferred_element_type=F32)


def first_kernel(words_ref, table_ref, x_ref, out_ref):
    write_lines(x_ref[...], words_ref, table_ref, out_ref)


def top_kernel(words_ref, weights_ref, x_ref, top_ref):
    top_ref[...] = rotated(words_ref, weights_ref, x_ref, slice(0, top_ref.shape[1]))


def bottom_kernel(words_ref, weights_ref, x_ref, top_ref, y_ref):
    width = top_ref.shape[1]
    y_ref[:, :width] = top_ref[...]
    y_ref[:, width:] = rotated(words_ref, weights_ref, x_ref, slice(width, 2 * width))


def joined_kernel(words_ref, weights_ref, x_ref, top_ref, next_words_ref, next_table_ref, out_ref, y_ref):
    bottom_kernel(words_ref, weights_ref, x_ref, top_ref, y_ref)
    write_lines(y_ref[...], next_words_ref, next_table_ref, out_ref)


def call(kernel, outs, *args, scratch=()):
    shapes = [jax.ShapeDtypeStruct(shape, dtype) for shape, dtype in outs]
    single = len(shapes) == 1
    return pl.pallas_call(
        kernel,
        out_shape=shapes[0] if single else shapes,
        scratch_shapes=[pltpu.VMEM(shape, F32) for shape in scratch],
        compiler_params=pltpu.CompilerParams(vmem_limit_bytes=VMEM_BYTES),
    )(*args)


def exchanged(value, axis):
    return lax.all_to_all(value, axis, split_axis=0, concat_axis=0, tiled=True)


def passed_along(block, axis, distance):
    devices = range(lax.axis_size(axis))
    route = [((i - distance) % len(devices), i) for i in devices]
    return lax.ppermute(block, axis, route)


def body(matrix, plan):
    rows, owners, halves, width = matrix.shape
    peers = lax.axis_size(SUMMED)
    across = halves * width
    flat = ((rows * owners, across), F32)
    half = ((rows * owners, width), F32)
    sorted_rows = ((owners, rows, across), F32)
    sent = ((peers, LINES, across), F32)
    weights_shape = ((WORDS, across), F32)
    scratch = [(LINES, across), (ROUNDS, LINES, across), (16, across)]
    lines = matrix.reshape(rows * owners * halves, width)
    x = exchanged(call(sort_kernel, [sorted_rows], lines), OWNERS).reshape(flat[0])
    words_shape = ((WORDS, across), jnp.int32)
    table_shape = ((across, (WORDS - 1) * across), BF16)
    plans = call(plan_kernel, [words_shape] * STEPS + [table_shape] * STEPS, plan.reshape(-1, across))
    words, tables = plans[:STEPS], plans[STEPS:]
    part = call(first_kernel, [sent], words[0], tables[0], x)
    for step in range(STEPS):
        x_before = passed_along(x, "cols", 1)
        part = exchanged(part, SUMMED)
        weights = call(angles_kernel, [weights_shape], words[step], tables[step], part, scratch=scratch)
        weights_before = passed_along(weights, "cols", 1)
        top = call(top_kernel, [half], words[step], weights, x)
        args = (words[step], weights_before, x_before, top)
        if step + 1 < STEPS:
            part, x = call(joined_kernel, [sent, flat], *args, words[step + 1], tables[step + 1])
        else:
            x = call(bottom_kernel, [flat], *args)
    x = exchanged(x.reshape(sorted_rows[0]), OWNERS)
    return call(unsort_kernel, [(lines.shape, F32)], x).reshape(matrix.shape)


def solution(mesh):
    split = Mesh(mesh.devices.reshape(4, 8, 2, mesh.shape["cols"]), ("x", "z", "yh", "cols"))
    in_specs = (P(ROWS, "cols", None, None), P())
    out_specs = P(ROWS, "cols", None, None)
    return jax.shard_map(body, mesh=split, in_specs=in_specs, out_specs=out_specs, check_vma=False)
```

```python
import jax
import jax.numpy as jnp
from jax import lax
from jax.experimental import pallas as pl
from jax.experimental.pallas import tpu as pltpu
from jax.sharding import Mesh
from jax.sharding import PartitionSpec as P

STEPS = 2
ROWS = ("x", "z", "yh")
OWNERS = ("x", "yh")
SUMMED = "z"
ROUNDS = 4
WORDS = 1 << ROUNDS
LINES = 56
VMEM_BYTES = 16 * 1024 * 1024
F32 = jnp.float32
BF16 = jnp.bfloat16


def one_hot(partner):
    width = partner.shape[1]
    return lax.broadcasted_iota(jnp.int32, (width, width), 0) == partner


def pieces(value):
    high = value.astype(BF16)
    rest = value - high.astype(F32)
    middle = rest.astype(BF16)
    return high, middle, (rest - middle.astype(F32)).astype(BF16)


def permuted(value, table):
    return sum(jnp.dot(part, table, preferred_element_type=F32) for part in pieces(value))


def angle(orient, own, other, cross):
    spread = orient * (other - own)
    sign = jnp.where(spread >= 0.0, 1.0, -1.0)
    tangent = sign * 2.0 * cross / (jnp.abs(spread) + jnp.sqrt(spread * spread + 4.0 * cross * cross))
    cosine = 1.0 / jnp.sqrt(1.0 + tangent * tangent)
    return cosine, -orient * (tangent * cosine)


def write_lines(x, words_ref, out_ref, moved_ref, lines_ref):
    width = x.shape[1]
    gram = lax.dot_general(
        x, x, (((0,), (0,)), ((), ())), precision=lax.Precision.HIGHEST, preferred_element_type=F32
    )
    parts = pieces(gram)
    moved_ref[0] = gram
    for left in range(1, moved_ref.shape[0]):
        table = one_hot(words_ref[left : left + 1]).astype(BF16)
        moved_ref[left] = sum(jnp.dot(part, table, preferred_element_type=F32) for part in parts)
    line = lax.broadcasted_iota(jnp.int32, (8, width), 0)

    def pick(word, places):
        row = words_ref[word : word + 1]
        found = [jnp.zeros((8, width), F32) for _ in places]
        for start in range(0, width, 8):
            here = line == row - start
            for i in range(len(places)):
                found[i] = jnp.where(here, moved_ref[i, start : start + 8], found[i])
        for value, place in zip(found, places):
            lines_ref[place : place + 1] = value.sum(axis=0, keepdims=True)

    lines_ref[LINES - 8 :] = jnp.zeros((8, width), F32)
    pick(0, [0])
    for number in range(ROUNDS):
        for right in range(1 << number):
            pick((1 << number) + right, [place_of(number, left, right) for left in range(right + 1)])
    lines = lines_ref[...]
    for i in range(out_ref.shape[0]):
        out_ref[i] = lines


def place_of(number, left, right):
    return 1 + sum((1 << i) * ((1 << i) + 1) // 2 for i in range(number)) + right * (right + 1) // 2 + left


def table_of(words_ref, number):
    count = 1 << number
    return one_hot(words_ref[count : count + 1]).astype(BF16)


def angles_kernel(words_ref, part_ref, out_ref, lines_ref, moved_ref, state_ref):
    width = words_ref.shape[1]
    lines = jnp.sum(part_ref[...], axis=0)
    lines_ref[...] = lines
    split = pieces(lines)
    tables = [table_of(words_ref, number) for number in range(ROUNDS)]
    for number, table in enumerate(tables):
        moved_ref[number] = sum(jnp.dot(part, table, preferred_element_type=F32) for part in split)
    indices = lax.broadcasted_iota(jnp.int32, (1, width), 1)
    state_ref[...] = jnp.zeros_like(state_ref)
    diag, diag_2 = lines_ref[:1], moved_ref[0, :1]
    weights, weights_2 = [jnp.ones((1, width), F32)], [jnp.ones((1, width), F32)]
    for number in range(ROUNDS):
        count = 1 << number
        if number:
            for i, value in enumerate([diag] + weights):
                state_ref[i : i + 1] = value
            other = permuted(state_ref[...], tables[number])
            diag_2, *weights_2 = (other[i : i + 1] for i in range(1 + count))
        cross = jnp.zeros((1, width), F32)
        for left in range(count):
            inner = jnp.zeros((1, width), F32)
            for right in range(count):
                place = place_of(number, min(left, right), max(left, right))
                source = lines_ref[place : place + 1] if left <= right else moved_ref[number, place : place + 1]
                inner += weights_2[right] * source
            cross += weights[left] * inner
        orient = jnp.where(indices < words_ref[count : count + 1], 1.0, -1.0)
        cos, sin = angle(orient, diag, diag_2, cross)
        diag = cos * cos * diag + 2.0 * cos * sin * cross + sin * sin * diag_2
        weights = [cos * value for value in weights] + [sin * value for value in weights_2]
    for i, value in enumerate(weights):
        out_ref[i : i + 1] = value


def plan_kernel(plan_ref, *words_refs):
    width = plan_ref.shape[1]
    for step, words_ref in enumerate(words_refs):
        words = lax.broadcasted_iota(jnp.int32, (1, width), 1)
        for number in range(ROUNDS):
            partner = plan_ref[step * ROUNDS + number : step * ROUNDS + number + 1]
            known = jnp.concatenate([words] * (WORDS // words.shape[0]), axis=0).astype(F32).astype(BF16)
            moved = jnp.dot(known, one_hot(partner).astype(BF16), preferred_element_type=F32)
            words = jnp.concatenate([words, moved[: words.shape[0]].astype(jnp.int32)], axis=0)
        words_ref[...] = words


def sort_kernel(in_ref, out_ref):
    rows, owners = out_ref.shape[1], out_ref.shape[0]
    for i in range(owners):
        for half in range(2):
            out_ref[i, :, half * 128 : half * 128 + 128] = in_ref[pl.ds(2 * i + half, rows, 2 * owners), :]


def unsort_kernel(in_ref, out_ref):
    rows, owners = in_ref.shape[1], in_ref.shape[0]
    for i in range(owners):
        for half in range(2):
            out_ref[pl.ds(2 * i + half, rows, 2 * owners), :] = in_ref[i, :, half * 128 : half * 128 + 128]


def rotated(words_ref, weights_ref, x_ref, columns):
    line = lax.broadcasted_iota(jnp.int32, (x_ref.shape[1], columns.stop - columns.start), 0)
    rotation = jnp.zeros(line.shape, F32)
    for i in range(WORDS):
        rotation += jnp.where(line == words_ref[i : i + 1, columns], weights_ref[i : i + 1, columns], 0.0)
    return jnp.dot(x_ref[...], rotation, precision=lax.Precision.HIGHEST, preferred_element_type=F32)


def first_kernel(words_ref, x_ref, out_ref, moved_ref, lines_ref):
    write_lines(x_ref[...], words_ref, out_ref, moved_ref, lines_ref)


def top_kernel(words_ref, weights_ref, x_ref, top_ref):
    top_ref[...] = rotated(words_ref, weights_ref, x_ref, slice(0, top_ref.shape[1]))


def bottom_kernel(words_ref, weights_ref, x_ref, top_ref, y_ref):
    width = top_ref.shape[1]
    y_ref[:, :width] = top_ref[...]
    y_ref[:, width:] = rotated(words_ref, weights_ref, x_ref, slice(width, 2 * width))


def joined_kernel(
    words_ref, weights_ref, x_ref, top_ref, next_words_ref, out_ref, y_ref, moved_ref, lines_ref
):
    bottom_kernel(words_ref, weights_ref, x_ref, top_ref, y_ref)
    write_lines(y_ref[...], next_words_ref, out_ref, moved_ref, lines_ref)


def call(kernel, outs, *args, scratch=()):
    shapes = [jax.ShapeDtypeStruct(shape, dtype) for shape, dtype in outs]
    single = len(shapes) == 1
    return pl.pallas_call(
        kernel,
        out_shape=shapes[0] if single else shapes,
        scratch_shapes=[pltpu.VMEM(shape, F32) for shape in scratch],
        compiler_params=pltpu.CompilerParams(vmem_limit_bytes=VMEM_BYTES),
    )(*args)


def exchanged(value, axis):
    return lax.all_to_all(value, axis, split_axis=0, concat_axis=0, tiled=True)


def passed_along(block, axis, distance):
    devices = range(lax.axis_size(axis))
    route = [((i - distance) % len(devices), i) for i in devices]
    return lax.ppermute(block, axis, route)


def body(matrix, plan):
    rows, owners, halves, width = matrix.shape
    peers = lax.axis_size(SUMMED)
    across = halves * width
    flat = ((rows * owners, across), F32)
    half = ((rows * owners, width), F32)
    sorted_rows = ((owners, rows, across), F32)
    sent = ((peers, LINES, across), F32)
    weights_shape = ((WORDS, across), F32)
    scratch = [(LINES, across), (ROUNDS, LINES, across), (16, across)]
    lines = matrix.reshape(rows * owners * halves, width)
    x = exchanged(call(sort_kernel, [sorted_rows], lines), OWNERS).reshape(flat[0])
    words_shape = ((WORDS, across), jnp.int32)
    cut = [(WORDS // 2, across, across), (LINES, across)]
    words = call(plan_kernel, [words_shape] * STEPS, plan.reshape(-1, across))
    part = call(first_kernel, [sent], words[0], x, scratch=cut)
    for step in range(STEPS):
        x_before = passed_along(x, "cols", 1)
        part = exchanged(part, SUMMED)
        weights = call(angles_kernel, [weights_shape], words[step], part, scratch=scratch)
        weights_before = passed_along(weights, "cols", 1)
        top = call(top_kernel, [half], words[step], weights, x)
        args = (words[step], weights_before, x_before, top)
        if step + 1 < STEPS:
            part, x = call(joined_kernel, [sent, flat], *args, words[step + 1], scratch=cut)
        else:
            x = call(bottom_kernel, [flat], *args)
    x = exchanged(x.reshape(sorted_rows[0]), OWNERS)
    return call(unsort_kernel, [(lines.shape, F32)], x).reshape(matrix.shape)


def solution(mesh):
    split = Mesh(mesh.devices.reshape(4, 8, 2, mesh.shape["cols"]), ("x", "z", "yh", "cols"))
    in_specs = (P(ROWS, "cols", None, None), P())
    out_specs = P(ROWS, "cols", None, None)
    return jax.shard_map(body, mesh=split, in_specs=in_specs, out_specs=out_specs, check_vma=False)
```

```python
import jax
import jax.numpy as jnp
from jax import lax
from jax.experimental import pallas as pl
from jax.experimental.pallas import tpu as pltpu
from jax.sharding import Mesh
from jax.sharding import PartitionSpec as P

STEPS = 2
ROWS = ("x", "z", "yh")
OWNERS = ("x", "yh")
SUMMED = "z"
ROUNDS = 4
WORDS = 1 << ROUNDS
LINES = 56
VMEM_BYTES = 16 * 1024 * 1024
F32 = jnp.float32
BF16 = jnp.bfloat16


def one_hot(partner):
    width = partner.shape[1]
    return lax.broadcasted_iota(jnp.int32, (width, width), 0) == partner


def pieces(value):
    high = value.astype(BF16)
    rest = value - high.astype(F32)
    middle = rest.astype(BF16)
    return high, middle, (rest - middle.astype(F32)).astype(BF16)


def permuted(value, table):
    return sum(jnp.dot(part, table, preferred_element_type=F32) for part in pieces(value))


def angle(orient, own, other, cross):
    spread = orient * (other - own)
    sign = jnp.where(spread >= 0.0, 1.0, -1.0)
    tangent = sign * 2.0 * cross / (jnp.abs(spread) + jnp.sqrt(spread * spread + 4.0 * cross * cross))
    cosine = 1.0 / jnp.sqrt(1.0 + tangent * tangent)
    return cosine, -orient * (tangent * cosine)


def write_lines(x, words_ref, out_ref, moved_ref, lines_ref):
    width = x.shape[1]
    gram = lax.dot_general(
        x, x, (((0,), (0,)), ((), ())), precision=lax.Precision.HIGHEST, preferred_element_type=F32
    )
    parts = pieces(gram)
    moved_ref[0] = gram
    for left in range(1, moved_ref.shape[0]):
        table = one_hot(words_ref[left : left + 1]).astype(BF16)
        moved_ref[left] = sum(jnp.dot(part, table, preferred_element_type=F32) for part in parts)
    line = lax.broadcasted_iota(jnp.int32, (8, width), 0)

    def pick(word, places):
        row = words_ref[word : word + 1]
        found = [jnp.zeros((8, width), F32) for _ in places]
        for start in range(0, width, 8):
            here = line == row - start
            for i in range(len(places)):
                found[i] = jnp.where(here, moved_ref[i, start : start + 8], found[i])
        for value, place in zip(found, places):
            lines_ref[place : place + 1] = value.sum(axis=0, keepdims=True)

    lines_ref[LINES - 8 :] = jnp.zeros((8, width), F32)
    pick(0, [0])
    for number in range(ROUNDS):
        for right in range(1 << number):
            pick((1 << number) + right, [place_of(number, left, right) for left in range(right + 1)])
    lines = lines_ref[...]
    for i in range(out_ref.shape[0]):
        out_ref[i] = lines


def place_of(number, left, right):
    return 1 + sum((1 << i) * ((1 << i) + 1) // 2 for i in range(number)) + right * (right + 1) // 2 + left


def table_of(words_ref, number):
    count = 1 << number
    return one_hot(words_ref[count : count + 1]).astype(BF16)


def angles_kernel(words_ref, part_ref, x_ref, out_ref, bottom_ref, lines_ref, moved_ref, state_ref):
    width = words_ref.shape[1]
    lines = jnp.sum(part_ref[...], axis=0)
    lines_ref[...] = lines
    split = pieces(lines)
    tables = [table_of(words_ref, number) for number in range(ROUNDS)]
    for number, table in enumerate(tables):
        moved_ref[number] = sum(jnp.dot(part, table, preferred_element_type=F32) for part in split)
    indices = lax.broadcasted_iota(jnp.int32, (1, width), 1)
    state_ref[...] = jnp.zeros_like(state_ref)
    diag, diag_2 = lines_ref[:1], moved_ref[0, :1]
    weights, weights_2 = [jnp.ones((1, width), F32)], [jnp.ones((1, width), F32)]
    for number in range(ROUNDS):
        count = 1 << number
        if number:
            for i, value in enumerate([diag] + weights):
                state_ref[i : i + 1] = value
            other = permuted(state_ref[...], tables[number])
            diag_2, *weights_2 = (other[i : i + 1] for i in range(1 + count))
        cross = jnp.zeros((1, width), F32)
        for left in range(count):
            inner = jnp.zeros((1, width), F32)
            for right in range(count):
                place = place_of(number, min(left, right), max(left, right))
                source = lines_ref[place : place + 1] if left <= right else moved_ref[number, place : place + 1]
                inner += weights_2[right] * source
            cross += weights[left] * inner
        orient = jnp.where(indices < words_ref[count : count + 1], 1.0, -1.0)
        cos, sin = angle(orient, diag, diag_2, cross)
        diag = cos * cos * diag + 2.0 * cos * sin * cross + sin * sin * diag_2
        weights = [cos * value for value in weights] + [sin * value for value in weights_2]
    for i, value in enumerate(weights):
        out_ref[i : i + 1] = value
    bottom_ref[...] = rotated(words_ref, out_ref, x_ref, slice(width - bottom_ref.shape[1], width))


def plan_kernel(plan_ref, *words_refs):
    width = plan_ref.shape[1]
    for step, words_ref in enumerate(words_refs):
        words = lax.broadcasted_iota(jnp.int32, (1, width), 1)
        for number in range(ROUNDS):
            partner = plan_ref[step * ROUNDS + number : step * ROUNDS + number + 1]
            known = jnp.concatenate([words] * (WORDS // words.shape[0]), axis=0).astype(F32).astype(BF16)
            moved = jnp.dot(known, one_hot(partner).astype(BF16), preferred_element_type=F32)
            words = jnp.concatenate([words, moved[: words.shape[0]].astype(jnp.int32)], axis=0)
        words_ref[...] = words


def sort_kernel(words_ref, in_ref, out_ref):
    del words_ref
    rows, owners = out_ref.shape[1], out_ref.shape[0]
    for i in range(owners):
        for half in range(2):
            out_ref[i, :, half * 128 : half * 128 + 128] = in_ref[pl.ds(2 * i + half, rows, 2 * owners), :]


def unsort_kernel(in_ref, out_ref):
    rows, owners = in_ref.shape[1], in_ref.shape[0]
    for i in range(owners):
        for half in range(2):
            out_ref[pl.ds(2 * i + half, rows, 2 * owners), :] = in_ref[i, :, half * 128 : half * 128 + 128]


def rotated(words_ref, weights_ref, x_ref, columns):
    line = lax.broadcasted_iota(jnp.int32, (x_ref.shape[1], columns.stop - columns.start), 0)
    rotation = jnp.zeros(line.shape, F32)
    for i in range(WORDS):
        rotation += jnp.where(line == words_ref[i : i + 1, columns], weights_ref[i : i + 1, columns], 0.0)
    return jnp.dot(x_ref[...], rotation, precision=lax.Precision.HIGHEST, preferred_element_type=F32)


def first_kernel(words_ref, x_ref, out_ref, moved_ref, lines_ref):
    write_lines(x_ref[...], words_ref, out_ref, moved_ref, lines_ref)


def top_kernel(words_ref, weights_ref, x_ref, top_ref):
    top_ref[...] = rotated(words_ref, weights_ref, x_ref, slice(0, top_ref.shape[1]))


def joined_kernel(words_ref, top_ref, bottom_ref, out_ref, y_ref, moved_ref, lines_ref):
    width = top_ref.shape[1]
    y_ref[:, :width] = top_ref[...]
    y_ref[:, width:] = bottom_ref[...]
    write_lines(y_ref[...], words_ref, out_ref, moved_ref, lines_ref)


def call(kernel, outs, *args, scratch=()):
    shapes = [jax.ShapeDtypeStruct(shape, dtype) for shape, dtype in outs]
    single = len(shapes) == 1
    return pl.pallas_call(
        kernel,
        out_shape=shapes[0] if single else shapes,
        scratch_shapes=[pltpu.VMEM(shape, F32) for shape in scratch],
        compiler_params=pltpu.CompilerParams(vmem_limit_bytes=VMEM_BYTES),
    )(*args)


def exchanged(value, axis):
    return lax.all_to_all(value, axis, split_axis=0, concat_axis=0, tiled=True)


def passed_along(block, axis, distance):
    devices = range(lax.axis_size(axis))
    route = [((i - distance) % len(devices), i) for i in devices]
    return lax.ppermute(block, axis, route)


def body(matrix, plan):
    rows, owners, halves, width = matrix.shape
    peers = lax.axis_size(SUMMED)
    across = halves * width
    flat = ((rows * owners, across), F32)
    half = ((rows * owners, width), F32)
    sorted_rows = ((owners, rows, across), F32)
    sent = ((peers, LINES, across), F32)
    weights_shape = ((WORDS, across), F32)
    scratch = [(LINES, across), (ROUNDS, LINES, across), (16, across)]
    lines = matrix.reshape(rows * owners * halves, width)
    words_shape = ((WORDS, across), jnp.int32)
    cut = [(WORDS // 2, across, across), (LINES, across)]
    words = call(plan_kernel, [words_shape] * STEPS, plan.reshape(-1, across))
    x = exchanged(call(sort_kernel, [sorted_rows], words[0], lines), OWNERS).reshape(flat[0])
    part = call(first_kernel, [sent], words[0], x, scratch=cut)
    for step in range(STEPS):
        part = exchanged(part, SUMMED)
        weights, bottom = call(angles_kernel, [weights_shape, half], words[step], part, x, scratch=scratch)
        bottom = passed_along(bottom, "cols", 1)
        top = call(top_kernel, [half], words[step], weights, x)
        if step + 1 < STEPS:
            part, x = call(joined_kernel, [sent, flat], words[step + 1], top, bottom, scratch=cut)
    x = exchanged(jnp.concatenate([top, bottom], axis=1).reshape(sorted_rows[0]), OWNERS)
    return call(unsort_kernel, [(lines.shape, F32)], x).reshape(matrix.shape)


def solution(mesh):
    split = Mesh(mesh.devices.reshape(4, 8, 2, mesh.shape["cols"]), ("x", "z", "yh", "cols"))
    in_specs = (P(ROWS, "cols", None, None), P())
    out_specs = P(ROWS, "cols", None, None)
    return jax.shard_map(body, mesh=split, in_specs=in_specs, out_specs=out_specs, check_vma=False)
```

```python
import jax
import jax.numpy as jnp
from jax import lax
from jax.experimental import pallas as pl
from jax.experimental.pallas import tpu as pltpu
from jax.sharding import Mesh
from jax.sharding import PartitionSpec as P

STEPS = 2
ROWS = ("x", "z", "yh")
OWNERS = ("x", "yh")
SUMMED = "z"
ROUNDS = 4
WORDS = 1 << ROUNDS
LINES = 48
CHUNKS = 4
VMEM_BYTES = 16 * 1024 * 1024
F32 = jnp.float32
BF16 = jnp.bfloat16


def one_hot(partner):
    width = partner.shape[1]
    return lax.broadcasted_iota(jnp.int32, (width, width), 0) == partner


def pieces(value):
    high = value.astype(BF16)
    rest = value - high.astype(F32)
    middle = rest.astype(BF16)
    return high, middle, (rest - middle.astype(F32)).astype(BF16)


def permuted(value, table):
    return sum(jnp.dot(part, table, preferred_element_type=F32) for part in pieces(value))


def angle(orient, own, other, cross):
    spread = orient * (other - own)
    sign = jnp.where(spread >= 0.0, 1.0, -1.0)
    tangent = sign * 2.0 * cross / (jnp.abs(spread) + jnp.sqrt(spread * spread + 4.0 * cross * cross))
    cosine = 1.0 / jnp.sqrt(1.0 + tangent * tangent)
    return cosine, -orient * (tangent * cosine)


def write_lines(x, words_ref, out_ref, moved_ref, lines_ref):
    width = x.shape[1]
    gram = lax.dot_general(
        x, x, (((0,), (0,)), ((), ())), precision=lax.Precision.HIGHEST, preferred_element_type=F32
    )
    parts = pieces(gram)
    moved_ref[0] = gram
    for left in range(1, moved_ref.shape[0]):
        table = one_hot(words_ref[left : left + 1]).astype(BF16)
        moved_ref[left] = sum(jnp.dot(part, table, preferred_element_type=F32) for part in parts)
    line = lax.broadcasted_iota(jnp.int32, (8, width), 0)

    def pick(word, count):
        row = words_ref[word : word + 1]
        found = [jnp.zeros((8, width), F32) for _ in range(count)]
        for start in range(0, width, 8):
            here = line == row - start
            for i in range(count):
                found[i] = jnp.where(here, moved_ref[i, start : start + 8], found[i])
        return [value.sum(axis=0, keepdims=True) for value in found]

    def store(place, value):
        lines_ref[place : place + 1] = value

    lines_ref[LINES - 8 :] = jnp.zeros((8, width), F32)
    store(0, pick(0, 1)[0])
    indices = lax.broadcasted_iota(jnp.int32, (1, width), 1)
    for number in range(ROUNDS):
        count = 1 << number
        first = indices < words_ref[count : count + 1]
        for right in range(count):
            *found, same = pick(count + right, right + 1)
            for left, value in enumerate(found):
                store(place_of(number, left, right), value)
            place = place_of(number, right, right)
            store(place, jnp.where(first, lines_ref[place : place + 1], same) if right % 2 else same)
    lines = lines_ref[...]
    for i in range(out_ref.shape[0]):
        out_ref[i] = lines


def place_of(number, left, right):
    count = 1 << number
    start = (0, 2, 4, 12)[number] if number else 1
    if left == right:
        return start + count * (count - 1) // 2 + left // 2
    return start + right * (right - 1) // 2 + left


def table_of(words_ref, number):
    count = 1 << number
    return one_hot(words_ref[count : count + 1]).astype(BF16)


def angles_kernel(words_ref, part_ref, out_ref, lines_ref, moved_ref, state_ref):
    width = words_ref.shape[1]
    lines = jnp.sum(part_ref[...], axis=0)
    lines_ref[...] = lines
    split = pieces(lines)
    tables = [table_of(words_ref, number) for number in range(ROUNDS)]
    for number, table in enumerate(tables):
        moved_ref[number] = sum(jnp.dot(part, table, preferred_element_type=F32) for part in split)
    indices = lax.broadcasted_iota(jnp.int32, (1, width), 1)
    state_ref[...] = jnp.zeros_like(state_ref)
    diag, diag_2 = lines_ref[:1], moved_ref[0, :1]
    weights, weights_2 = [jnp.ones((1, width), F32)], [jnp.ones((1, width), F32)]
    for number in range(ROUNDS):
        count = 1 << number
        if number:
            for i, value in enumerate([diag] + weights):
                state_ref[i : i + 1] = value
            other = permuted(state_ref[...], tables[number])
            diag_2, *weights_2 = (other[i : i + 1] for i in range(1 + count))
        first = indices < words_ref[count : count + 1]
        cross = jnp.zeros((1, width), F32)
        for left in range(count):
            inner = jnp.zeros((1, width), F32)
            for right in range(count):
                place = place_of(number, min(left, right), max(left, right))
                line, moved = lines_ref[place : place + 1], moved_ref[number, place : place + 1]
                if left == right and number:
                    line = jnp.where(first, moved, line) if left % 2 else jnp.where(first, line, moved)
                inner += weights_2[right] * (line if left <= right else moved)
            cross += weights[left] * inner
        orient = jnp.where(first, 1.0, -1.0)
        cos, sin = angle(orient, diag, diag_2, cross)
        diag = cos * cos * diag + 2.0 * cos * sin * cross + sin * sin * diag_2
        weights = [cos * value for value in weights] + [sin * value for value in weights_2]
    for i, value in enumerate(weights):
        out_ref[i : i + 1] = value


def plan_kernel(plan_ref, *words_refs):
    width = plan_ref.shape[1]
    for step, words_ref in enumerate(words_refs):
        words = lax.broadcasted_iota(jnp.int32, (1, width), 1)
        for number in range(ROUNDS):
            partner = plan_ref[step * ROUNDS + number : step * ROUNDS + number + 1]
            known = jnp.concatenate([words] * (WORDS // words.shape[0]), axis=0).astype(F32).astype(BF16)
            moved = jnp.dot(known, one_hot(partner).astype(BF16), preferred_element_type=F32)
            words = jnp.concatenate([words, moved[: words.shape[0]].astype(jnp.int32)], axis=0)
        words_ref[...] = words


def sort_kernel(in_ref, out_ref, held_ref, ready_ref, in_sem, out_sem):
    owners = out_ref.shape[0]
    lines, rows = held_ref.shape[1], ready_ref.shape[2]
    reads = [
        pltpu.make_async_copy(in_ref.at[pl.ds(i * lines, lines)], held_ref.at[i], in_sem.at[i]) for i in range(CHUNKS)
    ]
    writes = [
        pltpu.make_async_copy(ready_ref.at[i], out_ref.at[:, pl.ds(i * rows, rows)], out_sem.at[i])
        for i in range(CHUNKS)
    ]
    for read in reads:
        read.start()
    for i in range(CHUNKS):
        reads[i].wait()
        for j in range(2 * owners):
            half = j % 2 * 128
            ready_ref[i, j // 2, :, half : half + 128] = held_ref[i, pl.ds(j, rows, 2 * owners), :]
        writes[i].start()
    for write in writes:
        write.wait()


def unsort_kernel(in_ref, out_ref, ready_ref, out_sem):
    owners = in_ref.shape[0]
    lines = ready_ref.shape[1]
    rows = lines // (2 * owners)
    writes = [
        pltpu.make_async_copy(ready_ref.at[i], out_ref.at[pl.ds(i * lines, lines)], out_sem.at[i])
        for i in range(CHUNKS)
    ]
    for i in range(CHUNKS):
        for j in range(2 * owners):
            half = j % 2 * 128
            ready_ref[i, pl.ds(j, rows, 2 * owners), :] = in_ref[
                j // 2, i * rows : i * rows + rows, half : half + 128
            ]
        writes[i].start()
    for write in writes:
        write.wait()


def sorted_rows_of(lines, shape):
    owners, rows, across = shape
    return pl.pallas_call(
        sort_kernel,
        out_shape=pltpu.HBM(shape, F32),
        in_specs=[pl.BlockSpec(memory_space=pltpu.HBM)],
        out_specs=pl.BlockSpec(memory_space=pltpu.HBM),
        scratch_shapes=[
            pltpu.VMEM((CHUNKS, lines.shape[0] // CHUNKS, lines.shape[1]), F32),
            pltpu.VMEM((CHUNKS, owners, rows // CHUNKS, across), F32),
            pltpu.SemaphoreType.DMA((CHUNKS,)),
            pltpu.SemaphoreType.DMA((CHUNKS,)),
        ],
        compiler_params=pltpu.CompilerParams(vmem_limit_bytes=VMEM_BYTES),
    )(pltpu.with_memory_space_constraint(lines, pltpu.HBM))


def lines_from(value, shape):
    return pl.pallas_call(
        unsort_kernel,
        out_shape=pltpu.HBM(shape, F32),
        out_specs=pl.BlockSpec(memory_space=pltpu.HBM),
        scratch_shapes=[
            pltpu.VMEM((CHUNKS, shape[0] // CHUNKS, shape[1]), F32),
            pltpu.SemaphoreType.DMA((CHUNKS,)),
        ],
        compiler_params=pltpu.CompilerParams(vmem_limit_bytes=VMEM_BYTES),
    )(value)


def rotated(words_ref, weights_ref, x_ref, columns):
    line = lax.broadcasted_iota(jnp.int32, (x_ref.shape[1], columns.stop - columns.start), 0)
    rotation = jnp.zeros(line.shape, F32)
    for i in range(WORDS):
        rotation += jnp.where(line == words_ref[i : i + 1, columns], weights_ref[i : i + 1, columns], 0.0)
    return jnp.dot(x_ref[...], rotation, precision=lax.Precision.HIGHEST, preferred_element_type=F32)


def first_kernel(words_ref, x_ref, out_ref, moved_ref, lines_ref):
    write_lines(x_ref[...], words_ref, out_ref, moved_ref, lines_ref)


def top_kernel(words_ref, weights_ref, x_ref, top_ref):
    top_ref[...] = rotated(words_ref, weights_ref, x_ref, slice(0, top_ref.shape[1]))


def bottom_kernel(words_ref, weights_ref, x_ref, top_ref, y_ref):
    width = top_ref.shape[1]
    y_ref[:, :width] = top_ref[...]
    y_ref[:, width:] = rotated(words_ref, weights_ref, x_ref, slice(width, 2 * width))


def joined_kernel(
    words_ref, weights_ref, x_ref, top_ref, next_words_ref, out_ref, y_ref, moved_ref, lines_ref
):
    bottom_kernel(words_ref, weights_ref, x_ref, top_ref, y_ref)
    write_lines(y_ref[...], next_words_ref, out_ref, moved_ref, lines_ref)


def call(kernel, outs, *args, scratch=()):
    shapes = [jax.ShapeDtypeStruct(shape, dtype) for shape, dtype in outs]
    single = len(shapes) == 1
    return pl.pallas_call(
        kernel,
        out_shape=shapes[0] if single else shapes,
        scratch_shapes=[pltpu.VMEM(shape, F32) for shape in scratch],
        compiler_params=pltpu.CompilerParams(vmem_limit_bytes=VMEM_BYTES),
    )(*args)


def exchanged(value, axis):
    return lax.all_to_all(value, axis, split_axis=0, concat_axis=0, tiled=True)


def passed_along(block, axis, distance):
    devices = range(lax.axis_size(axis))
    route = [((i - distance) % len(devices), i) for i in devices]
    return lax.ppermute(block, axis, route)


def body(matrix, plan):
    rows, owners, halves, width = matrix.shape
    peers = lax.axis_size(SUMMED)
    across = halves * width
    flat = ((rows * owners, across), F32)
    half = ((rows * owners, width), F32)
    sorted_rows = (owners, rows, across)
    sent = ((peers, LINES, across), F32)
    weights_shape = ((WORDS, across), F32)
    scratch = [(LINES, across), (ROUNDS, LINES, across), (16, across)]
    lines = matrix.reshape(rows * owners * halves, width)
    x = exchanged(sorted_rows_of(lines, sorted_rows), OWNERS).reshape(flat[0])
    words_shape = ((WORDS, across), jnp.int32)
    cut = [(WORDS // 2, across, across), (LINES, across)]
    words = call(plan_kernel, [words_shape] * STEPS, plan.reshape(-1, across))
    part = call(first_kernel, [sent], words[0], x, scratch=cut)
    for step in range(STEPS):
        x_before = passed_along(x, "cols", 1)
        part = exchanged(part, SUMMED)
        weights = call(angles_kernel, [weights_shape], words[step], part, scratch=scratch)
        weights_before = passed_along(weights, "cols", 1)
        top = call(top_kernel, [half], words[step], weights, x)
        args = (words[step], weights_before, x_before, top)
        if step + 1 < STEPS:
            part, x = call(joined_kernel, [sent, flat], *args, words[step + 1], scratch=cut)
        else:
            x = call(bottom_kernel, [flat], *args)
    x = exchanged(x.reshape(sorted_rows), OWNERS)
    return lines_from(x, lines.shape).reshape(matrix.shape)


def solution(mesh):
    split = Mesh(mesh.devices.reshape(4, 8, 2, mesh.shape["cols"]), ("x", "z", "yh", "cols"))
    in_specs = (P(ROWS, "cols", None, None), P())
    out_specs = P(ROWS, "cols", None, None)
    return jax.shard_map(body, mesh=split, in_specs=in_specs, out_specs=out_specs, check_vma=False)
```

```python
import jax
import jax.numpy as jnp
from jax import lax
from jax.experimental import pallas as pl
from jax.experimental.pallas import tpu as pltpu
from jax.sharding import Mesh
from jax.sharding import PartitionSpec as P

STEPS = 2
ROWS = ("x", "z", "yh")
OWNERS = ("x", "yh")
SUMMED = "z"
ROUNDS = 4
WORDS = 1 << ROUNDS
LINES = 44
SENT = ((0, 24), (24, 64), (64, 88))
CHUNKS = 4
VMEM_BYTES = 16 * 1024 * 1024
F32 = jnp.float32
BF16 = jnp.bfloat16


def one_hot(partner):
    width = partner.shape[1]
    return lax.broadcasted_iota(jnp.int32, (width, width), 0) == partner


def pieces(value):
    high = value.astype(BF16)
    rest = value - high.astype(F32)
    middle = rest.astype(BF16)
    return high, middle, (rest - middle.astype(F32)).astype(BF16)


def permuted(value, table):
    return sum(jnp.dot(part, table, preferred_element_type=F32) for part in pieces(value))


def angle(orient, own, other, cross):
    spread = orient * (other - own)
    sign = jnp.where(spread >= 0.0, 1.0, -1.0)
    tangent = sign * 2.0 * cross / (jnp.abs(spread) + jnp.sqrt(spread * spread + 4.0 * cross * cross))
    cosine = 1.0 / jnp.sqrt(1.0 + tangent * tangent)
    return cosine, -orient * (tangent * cosine)


def write_lines(x, words_ref, out_ref, moved_ref, lines_ref, sem):
    width = x.shape[1]
    gram = lax.dot_general(
        x, x, (((0,), (0,)), ((), ())), precision=lax.Precision.HIGHEST, preferred_element_type=F32
    )
    parts = pieces(gram)
    moved_ref[0] = gram
    for left in range(1, moved_ref.shape[0]):
        table = one_hot(words_ref[left : left + 1]).astype(BF16)
        moved_ref[left] = sum(jnp.dot(part, table, preferred_element_type=F32) for part in parts)
    line = lax.broadcasted_iota(jnp.int32, (8, width), 0)

    def pick(word, count):
        row = words_ref[word : word + 1]
        found = [jnp.zeros((8, width), F32) for _ in range(count)]
        for start in range(0, width, 8):
            here = line == row - start
            for i in range(count):
                found[i] = jnp.where(here, moved_ref[i, start : start + 8], found[i])
        return [value.sum(axis=0, keepdims=True) for value in found]

    def store(place, value):
        lines_ref[2 * place : 2 * place + 1] = value[:, : width // 2]
        lines_ref[2 * place + 1 : 2 * place + 2] = value[:, width // 2 :]

    def loaded(place):
        halves = (lines_ref[2 * place : 2 * place + 1], lines_ref[2 * place + 1 : 2 * place + 2])
        return jnp.concatenate(halves, axis=1)

    copies = []

    def send(group):
        start, end = SENT[group]
        rows = pl.ds(start, end - start)
        for i in range(out_ref.shape[0]):
            copies.append(pltpu.make_async_copy(lines_ref.at[rows], out_ref.at[i, rows], sem.at[group, i]))
            copies[-1].start()

    store(0, pick(0, 1)[0])
    indices = lax.broadcasted_iota(jnp.int32, (1, width), 1)
    for number in range(ROUNDS):
        count = 1 << number
        first = indices < words_ref[count : count + 1]
        for right in range(count):
            *found, same = pick(count + right, right + 1)
            for left, value in enumerate(found):
                store(place_of(number, left, right), value)
            place = place_of(number, right, right)
            store(place, jnp.where(first, loaded(place), same) if right % 2 else same)
            if number == 3 and right == 6:
                send(1)
        if number == 2:
            send(0)
    send(2)
    for copy in copies:
        copy.wait()


def place_of(number, left, right):
    count = 1 << number
    start = (0, 2, 4, 12)[number] if number else 1
    if left == right:
        return start + count * (count - 1) // 2 + left // 2
    return start + right * (right - 1) // 2 + left


def table_of(words_ref, number):
    count = 1 << number
    return one_hot(words_ref[count : count + 1]).astype(BF16)


def angles_kernel(words_ref, part_ref, out_ref, sum_ref, lines_ref, moved_ref, state_ref):
    width = words_ref.shape[1]
    sum_ref[...] = jnp.sum(part_ref[...], axis=0)
    lines_ref[LINES:] = jnp.zeros((lines_ref.shape[0] - LINES, width), F32)
    for half in range(2):
        columns = slice(half * width // 2, (half + 1) * width // 2)
        lines_ref[:LINES, columns] = sum_ref[pl.ds(half, LINES, 2), :]
    split = pieces(lines_ref[...])
    tables = [table_of(words_ref, number) for number in range(ROUNDS)]
    for number, table in enumerate(tables):
        moved_ref[number] = sum(jnp.dot(part, table, preferred_element_type=F32) for part in split)
    indices = lax.broadcasted_iota(jnp.int32, (1, width), 1)
    state_ref[...] = jnp.zeros_like(state_ref)
    diag, diag_2 = lines_ref[:1], moved_ref[0, :1]
    weights, weights_2 = [jnp.ones((1, width), F32)], [jnp.ones((1, width), F32)]
    for number in range(ROUNDS):
        count = 1 << number
        if number:
            for i, value in enumerate([diag] + weights):
                state_ref[i : i + 1] = value
            other = permuted(state_ref[...], tables[number])
            diag_2, *weights_2 = (other[i : i + 1] for i in range(1 + count))
        first = indices < words_ref[count : count + 1]
        cross = jnp.zeros((1, width), F32)
        for left in range(count):
            inner = jnp.zeros((1, width), F32)
            for right in range(count):
                place = place_of(number, min(left, right), max(left, right))
                line, moved = lines_ref[place : place + 1], moved_ref[number, place : place + 1]
                if left == right and number:
                    line = jnp.where(first, moved, line) if left % 2 else jnp.where(first, line, moved)
                inner += weights_2[right] * (line if left <= right else moved)
            cross += weights[left] * inner
        orient = jnp.where(first, 1.0, -1.0)
        cos, sin = angle(orient, diag, diag_2, cross)
        diag = cos * cos * diag + 2.0 * cos * sin * cross + sin * sin * diag_2
        weights = [cos * value for value in weights] + [sin * value for value in weights_2]
    for i, value in enumerate(weights):
        out_ref[i : i + 1] = value


def plan_kernel(plan_ref, *words_refs):
    width = plan_ref.shape[1]
    for step, words_ref in enumerate(words_refs):
        words = lax.broadcasted_iota(jnp.int32, (1, width), 1)
        for number in range(ROUNDS):
            partner = plan_ref[step * ROUNDS + number : step * ROUNDS + number + 1]
            known = jnp.concatenate([words] * (WORDS // words.shape[0]), axis=0).astype(F32).astype(BF16)
            moved = jnp.dot(known, one_hot(partner).astype(BF16), preferred_element_type=F32)
            words = jnp.concatenate([words, moved[: words.shape[0]].astype(jnp.int32)], axis=0)
        words_ref[...] = words


def sort_kernel(in_ref, out_ref, held_ref, ready_ref, in_sem, out_sem):
    owners = out_ref.shape[0]
    lines, rows = held_ref.shape[1], ready_ref.shape[2]
    reads = [
        pltpu.make_async_copy(in_ref.at[pl.ds(i * lines, lines)], held_ref.at[i], in_sem.at[i]) for i in range(CHUNKS)
    ]
    writes = [
        pltpu.make_async_copy(ready_ref.at[i], out_ref.at[:, pl.ds(i * rows, rows)], out_sem.at[i])
        for i in range(CHUNKS)
    ]
    for read in reads:
        read.start()
    for i in range(CHUNKS):
        reads[i].wait()
        for j in range(2 * owners):
            half = j % 2 * 128
            ready_ref[i, j // 2, :, half : half + 128] = held_ref[i, pl.ds(j, rows, 2 * owners), :]
        writes[i].start()
    for write in writes:
        write.wait()


def unsort_kernel(in_ref, out_ref, ready_ref, out_sem):
    owners = in_ref.shape[0]
    lines = ready_ref.shape[1]
    rows = lines // (2 * owners)
    writes = [
        pltpu.make_async_copy(ready_ref.at[i], out_ref.at[pl.ds(i * lines, lines)], out_sem.at[i])
        for i in range(CHUNKS)
    ]
    for i in range(CHUNKS):
        for j in range(2 * owners):
            half = j % 2 * 128
            ready_ref[i, pl.ds(j, rows, 2 * owners), :] = in_ref[
                j // 2, i * rows : i * rows + rows, half : half + 128
            ]
        writes[i].start()
    for write in writes:
        write.wait()


def sorted_rows_of(lines, shape):
    owners, rows, across = shape
    return pl.pallas_call(
        sort_kernel,
        out_shape=pltpu.HBM(shape, F32),
        in_specs=[pl.BlockSpec(memory_space=pltpu.HBM)],
        out_specs=pl.BlockSpec(memory_space=pltpu.HBM),
        scratch_shapes=[
            pltpu.VMEM((CHUNKS, lines.shape[0] // CHUNKS, lines.shape[1]), F32),
            pltpu.VMEM((CHUNKS, owners, rows // CHUNKS, across), F32),
            pltpu.SemaphoreType.DMA((CHUNKS,)),
            pltpu.SemaphoreType.DMA((CHUNKS,)),
        ],
        compiler_params=pltpu.CompilerParams(vmem_limit_bytes=VMEM_BYTES),
    )(pltpu.with_memory_space_constraint(lines, pltpu.HBM))


def lines_from(value, shape):
    return pl.pallas_call(
        unsort_kernel,
        out_shape=pltpu.HBM(shape, F32),
        out_specs=pl.BlockSpec(memory_space=pltpu.HBM),
        scratch_shapes=[
            pltpu.VMEM((CHUNKS, shape[0] // CHUNKS, shape[1]), F32),
            pltpu.SemaphoreType.DMA((CHUNKS,)),
        ],
        compiler_params=pltpu.CompilerParams(vmem_limit_bytes=VMEM_BYTES),
    )(value)


def rotated(words_ref, weights_ref, x_ref, columns):
    line = lax.broadcasted_iota(jnp.int32, (x_ref.shape[1], columns.stop - columns.start), 0)
    rotation = jnp.zeros(line.shape, F32)
    for i in range(WORDS):
        rotation += jnp.where(line == words_ref[i : i + 1, columns], weights_ref[i : i + 1, columns], 0.0)
    return jnp.dot(x_ref[...], rotation, precision=lax.Precision.HIGHEST, preferred_element_type=F32)


def first_kernel(words_ref, x_ref, out_ref, moved_ref, lines_ref, sem):
    write_lines(x_ref[...], words_ref, out_ref, moved_ref, lines_ref, sem)


def top_kernel(words_ref, weights_ref, x_ref, top_ref):
    top_ref[...] = rotated(words_ref, weights_ref, x_ref, slice(0, top_ref.shape[1]))


def bottom_kernel(words_ref, weights_ref, x_ref, top_ref, y_ref):
    width = top_ref.shape[1]
    y_ref[:, :width] = top_ref[...]
    y_ref[:, width:] = rotated(words_ref, weights_ref, x_ref, slice(width, 2 * width))


def joined_kernel(
    words_ref, weights_ref, x_ref, top_ref, next_words_ref, out_ref, y_ref, moved_ref, lines_ref, sem
):
    bottom_kernel(words_ref, weights_ref, x_ref, top_ref, y_ref)
    write_lines(y_ref[...], next_words_ref, out_ref, moved_ref, lines_ref, sem)


def call(kernel, outs, *args, scratch=()):
    shapes = [jax.ShapeDtypeStruct(shape, dtype) for shape, dtype in outs]
    single = len(shapes) == 1
    return pl.pallas_call(
        kernel,
        out_shape=shapes[0] if single else shapes,
        scratch_shapes=[pltpu.VMEM(shape, F32) for shape in scratch],
        compiler_params=pltpu.CompilerParams(vmem_limit_bytes=VMEM_BYTES),
    )(*args)


def call_with_lines(kernel, sent, outs, *args):
    across = sent[1] * sent[2] // LINES
    return pl.pallas_call(
        kernel,
        out_shape=[pltpu.HBM(sent, F32)] + [jax.ShapeDtypeStruct(shape, F32) for shape in outs],
        out_specs=[pl.BlockSpec(memory_space=pltpu.HBM)] + [pl.BlockSpec(memory_space=pltpu.VMEM) for _ in outs],
        scratch_shapes=[
            pltpu.VMEM((WORDS // 2, across, across), F32),
            pltpu.VMEM(sent[1:], F32),
            pltpu.SemaphoreType.DMA((len(SENT), sent[0])),
        ],
        compiler_params=pltpu.CompilerParams(vmem_limit_bytes=VMEM_BYTES),
    )(*args)


def exchanged(value, axis):
    return lax.all_to_all(value, axis, split_axis=0, concat_axis=0, tiled=True)


def passed_along(block, axis, distance):
    devices = range(lax.axis_size(axis))
    route = [((i - distance) % len(devices), i) for i in devices]
    return lax.ppermute(block, axis, route)


def body(matrix, plan):
    rows, owners, halves, width = matrix.shape
    peers = lax.axis_size(SUMMED)
    across = halves * width
    flat = ((rows * owners, across), F32)
    half = ((rows * owners, width), F32)
    sorted_rows = (owners, rows, across)
    sent = (peers, 2 * LINES, across // 2)
    weights_shape = ((WORDS, across), F32)
    scratch = [sent[1:], (48, across), (ROUNDS, 48, across), (16, across)]
    lines = matrix.reshape(rows * owners * halves, width)
    x = exchanged(sorted_rows_of(lines, sorted_rows), OWNERS).reshape(flat[0])
    words_shape = ((WORDS, across), jnp.int32)
    words = call(plan_kernel, [words_shape] * STEPS, plan.reshape(-1, across))
    part = call_with_lines(first_kernel, sent, [], words[0], x)[0]
    for step in range(STEPS):
        x_before = passed_along(x, "cols", 1)
        part = exchanged(part, SUMMED)
        weights = call(angles_kernel, [weights_shape], words[step], part, scratch=scratch)
        weights_before = passed_along(weights, "cols", 1)
        top = call(top_kernel, [half], words[step], weights, x)
        args = (words[step], weights_before, x_before, top)
        if step + 1 < STEPS:
            part, x = call_with_lines(joined_kernel, sent, [flat[0]], *args, words[step + 1])
        else:
            x = call(bottom_kernel, [flat], *args)
    x = exchanged(x.reshape(sorted_rows), OWNERS)
    return lines_from(x, lines.shape).reshape(matrix.shape)


def solution(mesh):
    split = Mesh(mesh.devices.reshape(4, 8, 2, mesh.shape["cols"]), ("x", "z", "yh", "cols"))
    in_specs = (P(ROWS, "cols", None, None), P())
    out_specs = P(ROWS, "cols", None, None)
    return jax.shard_map(body, mesh=split, in_specs=in_specs, out_specs=out_specs, check_vma=False)
```

```python
import jax
import jax.numpy as jnp
from jax import lax
from jax.experimental import pallas as pl
from jax.experimental.pallas import tpu as pltpu
from jax.sharding import Mesh
from jax.sharding import PartitionSpec as P

STEPS = 2
ROWS = ("x", "z", "yh")
OWNERS = ("x", "yh")
SUMMED = "z"
ROUNDS = 4
WORDS = 1 << ROUNDS
LINES = 44
SENT = ((0, 24), (24, 64), (64, 88))
CHUNKS = 4
VMEM_BYTES = 16 * 1024 * 1024
F32 = jnp.float32
BF16 = jnp.bfloat16


def one_hot(partner):
    width = partner.shape[1]
    return lax.broadcasted_iota(jnp.int32, (width, width), 0) == partner


def pieces(value):
    high = value.astype(BF16)
    rest = value - high.astype(F32)
    middle = rest.astype(BF16)
    return high, middle, (rest - middle.astype(F32)).astype(BF16)


def product(left, right, contracted):
    (high, middle, _), (high_2, middle_2, _) = pieces(left), pieces(right)
    dims = (((contracted,), (0,)), ((), ()))
    pairs = ((high, middle_2), (middle, high_2), (high, high_2))
    return sum(lax.dot_general(a, b, dims, preferred_element_type=F32) for a, b in pairs)


def permuted(value, table):
    return sum(jnp.dot(part, table, preferred_element_type=F32) for part in pieces(value))


def angle(orient, own, other, cross):
    spread = orient * (other - own)
    sign = jnp.where(spread >= 0.0, 1.0, -1.0)
    tangent = sign * 2.0 * cross / (jnp.abs(spread) + jnp.sqrt(spread * spread + 4.0 * cross * cross))
    cosine = 1.0 / jnp.sqrt(1.0 + tangent * tangent)
    return cosine, -orient * (tangent * cosine)


def write_lines(x, words_ref, out_ref, moved_ref, lines_ref, sem):
    width = x.shape[1]
    gram = product(x, x, 0)
    parts = pieces(gram)
    moved_ref[0] = gram
    for left in range(1, moved_ref.shape[0]):
        table = one_hot(words_ref[left : left + 1]).astype(BF16)
        moved_ref[left] = sum(jnp.dot(part, table, preferred_element_type=F32) for part in parts)
    line = lax.broadcasted_iota(jnp.int32, (8, width), 0)

    def pick(word, count):
        row = words_ref[word : word + 1]
        found = [jnp.zeros((8, width), F32) for _ in range(count)]
        for start in range(0, width, 8):
            here = line == row - start
            for i in range(count):
                found[i] = jnp.where(here, moved_ref[i, start : start + 8], found[i])
        return [value.sum(axis=0, keepdims=True) for value in found]

    def store(place, value):
        lines_ref[2 * place : 2 * place + 1] = value[:, : width // 2]
        lines_ref[2 * place + 1 : 2 * place + 2] = value[:, width // 2 :]

    def loaded(place):
        halves = (lines_ref[2 * place : 2 * place + 1], lines_ref[2 * place + 1 : 2 * place + 2])
        return jnp.concatenate(halves, axis=1)

    copies = []

    def send(group):
        start, end = SENT[group]
        rows = pl.ds(start, end - start)
        for i in range(out_ref.shape[0]):
            copies.append(pltpu.make_async_copy(lines_ref.at[rows], out_ref.at[i, rows], sem.at[group, i]))
            copies[-1].start()

    store(0, pick(0, 1)[0])
    indices = lax.broadcasted_iota(jnp.int32, (1, width), 1)
    for number in range(ROUNDS):
        count = 1 << number
        first = indices < words_ref[count : count + 1]
        for right in range(count):
            *found, same = pick(count + right, right + 1)
            for left, value in enumerate(found):
                store(place_of(number, left, right), value)
            place = place_of(number, right, right)
            store(place, jnp.where(first, loaded(place), same) if right % 2 else same)
            if number == 3 and right == 6:
                send(1)
        if number == 2:
            send(0)
    send(2)
    for copy in copies:
        copy.wait()


def place_of(number, left, right):
    count = 1 << number
    start = (0, 2, 4, 12)[number] if number else 1
    if left == right:
        return start + count * (count - 1) // 2 + left // 2
    return start + right * (right - 1) // 2 + left


def table_of(words_ref, number):
    count = 1 << number
    return one_hot(words_ref[count : count + 1]).astype(BF16)


def angles_kernel(words_ref, part_ref, out_ref, sum_ref, lines_ref, moved_ref, state_ref):
    width = words_ref.shape[1]
    sum_ref[...] = jnp.sum(part_ref[...], axis=0)
    lines_ref[LINES:] = jnp.zeros((lines_ref.shape[0] - LINES, width), F32)
    for half in range(2):
        columns = slice(half * width // 2, (half + 1) * width // 2)
        lines_ref[:LINES, columns] = sum_ref[pl.ds(half, LINES, 2), :]
    split = pieces(lines_ref[...])
    tables = [table_of(words_ref, number) for number in range(ROUNDS)]
    for number, table in enumerate(tables):
        moved_ref[number] = sum(jnp.dot(part, table, preferred_element_type=F32) for part in split)
    indices = lax.broadcasted_iota(jnp.int32, (1, width), 1)
    state_ref[...] = jnp.zeros_like(state_ref)
    diag, diag_2 = lines_ref[:1], moved_ref[0, :1]
    weights, weights_2 = [jnp.ones((1, width), F32)], [jnp.ones((1, width), F32)]
    for number in range(ROUNDS):
        count = 1 << number
        if number:
            for i, value in enumerate([diag] + weights):
                state_ref[i : i + 1] = value
            other = permuted(state_ref[...], tables[number])
            diag_2, *weights_2 = (other[i : i + 1] for i in range(1 + count))
        first = indices < words_ref[count : count + 1]
        cross = jnp.zeros((1, width), F32)
        for left in range(count):
            inner = jnp.zeros((1, width), F32)
            for right in range(count):
                place = place_of(number, min(left, right), max(left, right))
                line, moved = lines_ref[place : place + 1], moved_ref[number, place : place + 1]
                if left == right and number:
                    line = jnp.where(first, moved, line) if left % 2 else jnp.where(first, line, moved)
                inner += weights_2[right] * (line if left <= right else moved)
            cross += weights[left] * inner
        orient = jnp.where(first, 1.0, -1.0)
        cos, sin = angle(orient, diag, diag_2, cross)
        diag = cos * cos * diag + 2.0 * cos * sin * cross + sin * sin * diag_2
        weights = [cos * value for value in weights] + [sin * value for value in weights_2]
    for i, value in enumerate(weights):
        out_ref[i : i + 1] = value


def plan_kernel(plan_ref, *words_refs):
    width = plan_ref.shape[1]
    for step, words_ref in enumerate(words_refs):
        words = lax.broadcasted_iota(jnp.int32, (1, width), 1)
        for number in range(ROUNDS):
            partner = plan_ref[step * ROUNDS + number : step * ROUNDS + number + 1]
            known = jnp.concatenate([words] * (WORDS // words.shape[0]), axis=0).astype(F32).astype(BF16)
            moved = jnp.dot(known, one_hot(partner).astype(BF16), preferred_element_type=F32)
            words = jnp.concatenate([words, moved[: words.shape[0]].astype(jnp.int32)], axis=0)
        words_ref[...] = words


def sort_kernel(in_ref, out_ref, held_ref, ready_ref, in_sem, out_sem):
    owners = out_ref.shape[0]
    lines, rows = held_ref.shape[1], ready_ref.shape[2]
    reads = [
        pltpu.make_async_copy(in_ref.at[pl.ds(i * lines, lines)], held_ref.at[i], in_sem.at[i]) for i in range(CHUNKS)
    ]
    writes = [
        pltpu.make_async_copy(ready_ref.at[i], out_ref.at[:, pl.ds(i * rows, rows)], out_sem.at[i])
        for i in range(CHUNKS)
    ]
    for read in reads:
        read.start()
    for i in range(CHUNKS):
        reads[i].wait()
        for j in range(2 * owners):
            half = j % 2 * 128
            ready_ref[i, j // 2, :, half : half + 128] = held_ref[i, pl.ds(j, rows, 2 * owners), :]
        writes[i].start()
    for write in writes:
        write.wait()


def unsort_kernel(in_ref, out_ref, ready_ref, out_sem):
    owners = in_ref.shape[0]
    lines = ready_ref.shape[1]
    rows = lines // (2 * owners)
    writes = [
        pltpu.make_async_copy(ready_ref.at[i], out_ref.at[pl.ds(i * lines, lines)], out_sem.at[i])
        for i in range(CHUNKS)
    ]
    for i in range(CHUNKS):
        for j in range(2 * owners):
            half = j % 2 * 128
            ready_ref[i, pl.ds(j, rows, 2 * owners), :] = in_ref[
                j // 2, i * rows : i * rows + rows, half : half + 128
            ]
        writes[i].start()
    for write in writes:
        write.wait()


def sorted_rows_of(lines, shape):
    owners, rows, across = shape
    return pl.pallas_call(
        sort_kernel,
        out_shape=pltpu.HBM(shape, F32),
        in_specs=[pl.BlockSpec(memory_space=pltpu.HBM)],
        out_specs=pl.BlockSpec(memory_space=pltpu.HBM),
        scratch_shapes=[
            pltpu.VMEM((CHUNKS, lines.shape[0] // CHUNKS, lines.shape[1]), F32),
            pltpu.VMEM((CHUNKS, owners, rows // CHUNKS, across), F32),
            pltpu.SemaphoreType.DMA((CHUNKS,)),
            pltpu.SemaphoreType.DMA((CHUNKS,)),
        ],
        compiler_params=pltpu.CompilerParams(vmem_limit_bytes=VMEM_BYTES),
    )(pltpu.with_memory_space_constraint(lines, pltpu.HBM))


def lines_from(value, shape):
    return pl.pallas_call(
        unsort_kernel,
        out_shape=pltpu.HBM(shape, F32),
        out_specs=pl.BlockSpec(memory_space=pltpu.HBM),
        scratch_shapes=[
            pltpu.VMEM((CHUNKS, shape[0] // CHUNKS, shape[1]), F32),
            pltpu.SemaphoreType.DMA((CHUNKS,)),
        ],
        compiler_params=pltpu.CompilerParams(vmem_limit_bytes=VMEM_BYTES),
    )(value)


def rotated(words_ref, weights_ref, x_ref, columns):
    line = lax.broadcasted_iota(jnp.int32, (x_ref.shape[1], columns.stop - columns.start), 0)
    rotation = jnp.zeros(line.shape, F32)
    for i in range(WORDS):
        rotation += jnp.where(line == words_ref[i : i + 1, columns], weights_ref[i : i + 1, columns], 0.0)
    return product(x_ref[...], rotation, 1)


def first_kernel(words_ref, x_ref, out_ref, moved_ref, lines_ref, sem):
    write_lines(x_ref[...], words_ref, out_ref, moved_ref, lines_ref, sem)


def top_kernel(words_ref, weights_ref, x_ref, top_ref):
    top_ref[...] = rotated(words_ref, weights_ref, x_ref, slice(0, top_ref.shape[1]))


def bottom_kernel(words_ref, weights_ref, x_ref, top_ref, y_ref):
    width = top_ref.shape[1]
    y_ref[:, :width] = top_ref[...]
    y_ref[:, width:] = rotated(words_ref, weights_ref, x_ref, slice(width, 2 * width))


def joined_kernel(
    words_ref, weights_ref, x_ref, top_ref, next_words_ref, out_ref, y_ref, moved_ref, lines_ref, sem
):
    bottom_kernel(words_ref, weights_ref, x_ref, top_ref, y_ref)
    write_lines(y_ref[...], next_words_ref, out_ref, moved_ref, lines_ref, sem)


def call(kernel, outs, *args, scratch=()):
    shapes = [jax.ShapeDtypeStruct(shape, dtype) for shape, dtype in outs]
    single = len(shapes) == 1
    return pl.pallas_call(
        kernel,
        out_shape=shapes[0] if single else shapes,
        scratch_shapes=[pltpu.VMEM(shape, F32) for shape in scratch],
        compiler_params=pltpu.CompilerParams(vmem_limit_bytes=VMEM_BYTES),
    )(*args)


def call_with_lines(kernel, sent, outs, *args):
    across = sent[1] * sent[2] // LINES
    return pl.pallas_call(
        kernel,
        out_shape=[pltpu.HBM(sent, F32)] + [jax.ShapeDtypeStruct(shape, F32) for shape in outs],
        out_specs=[pl.BlockSpec(memory_space=pltpu.HBM)] + [pl.BlockSpec(memory_space=pltpu.VMEM) for _ in outs],
        scratch_shapes=[
            pltpu.VMEM((WORDS // 2, across, across), F32),
            pltpu.VMEM(sent[1:], F32),
            pltpu.SemaphoreType.DMA((len(SENT), sent[0])),
        ],
        compiler_params=pltpu.CompilerParams(vmem_limit_bytes=VMEM_BYTES),
    )(*args)


def exchanged(value, axis):
    return lax.all_to_all(value, axis, split_axis=0, concat_axis=0, tiled=True)


def passed_along(block, axis, distance):
    devices = range(lax.axis_size(axis))
    route = [((i - distance) % len(devices), i) for i in devices]
    return lax.ppermute(block, axis, route)


def body(matrix, plan):
    rows, owners, halves, width = matrix.shape
    peers = lax.axis_size(SUMMED)
    across = halves * width
    flat = ((rows * owners, across), F32)
    half = ((rows * owners, width), F32)
    sorted_rows = (owners, rows, across)
    sent = (peers, 2 * LINES, across // 2)
    weights_shape = ((WORDS, across), F32)
    scratch = [sent[1:], (48, across), (ROUNDS, 48, across), (16, across)]
    lines = matrix.reshape(rows * owners * halves, width)
    x = exchanged(sorted_rows_of(lines, sorted_rows), OWNERS).reshape(flat[0])
    words_shape = ((WORDS, across), jnp.int32)
    words = call(plan_kernel, [words_shape] * STEPS, plan.reshape(-1, across))
    part = call_with_lines(first_kernel, sent, [], words[0], x)[0]
    for step in range(STEPS):
        x_before = passed_along(x, "cols", 1)
        part = exchanged(part, SUMMED)
        weights = call(angles_kernel, [weights_shape], words[step], part, scratch=scratch)
        weights_before = passed_along(weights, "cols", 1)
        top = call(top_kernel, [half], words[step], weights, x)
        args = (words[step], weights_before, x_before, top)
        if step + 1 < STEPS:
            part, x = call_with_lines(joined_kernel, sent, [flat[0]], *args, words[step + 1])
        else:
            x = call(bottom_kernel, [flat], *args)
    x = exchanged(x.reshape(sorted_rows), OWNERS)
    return lines_from(x, lines.shape).reshape(matrix.shape)


def solution(mesh):
    split = Mesh(mesh.devices.reshape(4, 8, 2, mesh.shape["cols"]), ("x", "z", "yh", "cols"))
    in_specs = (P(ROWS, "cols", None, None), P())
    out_specs = P(ROWS, "cols", None, None)
    return jax.shard_map(body, mesh=split, in_specs=in_specs, out_specs=out_specs, check_vma=False)
```

```python
import jax
import jax.numpy as jnp
from jax import lax
from jax.experimental import pallas as pl
from jax.experimental.pallas import tpu as pltpu
from jax.sharding import Mesh
from jax.sharding import PartitionSpec as P

STEPS = 2
ROWS = ("x", "z", "yh")
OWNERS = ("x", "yh")
SUMMED = "z"
ROUNDS = 4
WORDS = 1 << ROUNDS
LINES = 44
SENT = ((0, 64), (64, 88))
CHUNKS = 4
VMEM_BYTES = 16 * 1024 * 1024
F32 = jnp.float32
BF16 = jnp.bfloat16


def one_hot(partner):
    width = partner.shape[1]
    return lax.broadcasted_iota(jnp.int32, (width, width), 0) == partner


def pieces(value):
    high = value.astype(BF16)
    rest = value - high.astype(F32)
    middle = rest.astype(BF16)
    return high, middle, (rest - middle.astype(F32)).astype(BF16)


def product(left, right, contracted):
    (high, middle, _), (high_2, middle_2, _) = pieces(left), pieces(right)
    dims = (((contracted,), (0,)), ((), ()))
    pairs = ((high, middle_2), (middle, high_2), (high, high_2))
    return sum(lax.dot_general(a, b, dims, preferred_element_type=F32) for a, b in pairs)


def permuted(value, table):
    rows = value.shape[0]
    moved = jnp.dot(jnp.concatenate(pieces(value), axis=0), table, preferred_element_type=F32)
    return moved[:rows] + moved[rows : 2 * rows] + moved[2 * rows :]


def angle(orient, own, other, cross):
    spread = orient * (other - own)
    sign = jnp.where(spread >= 0.0, 1.0, -1.0)
    tangent = sign * 2.0 * cross / (jnp.abs(spread) + jnp.sqrt(spread * spread + 4.0 * cross * cross))
    cosine = 1.0 / jnp.sqrt(1.0 + tangent * tangent)
    return cosine, -orient * (tangent * cosine)


def write_lines(x, words_ref, out_ref, moved_ref, lines_ref, sem):
    width = x.shape[1]
    gram = product(x, x, 0)
    stacked = jnp.concatenate(pieces(gram), axis=0)
    moved_ref[0] = gram
    for left in range(1, moved_ref.shape[0]):
        table = one_hot(words_ref[left : left + 1]).astype(BF16)
        moved = jnp.dot(stacked, table, preferred_element_type=F32)
        moved_ref[left] = moved[:width] + moved[width : 2 * width] + moved[2 * width :]
    line = lax.broadcasted_iota(jnp.int32, (8, width), 0)

    def pick(word, count):
        row = words_ref[word : word + 1]
        found = [jnp.zeros((8, width), F32) for _ in range(count)]
        for start in range(0, width, 8):
            here = line == row - start
            for i in range(count):
                found[i] = jnp.where(here, moved_ref[i, start : start + 8], found[i])
        return [value.sum(axis=0, keepdims=True) for value in found]

    def store(place, value):
        lines_ref[2 * place : 2 * place + 1] = value[:, : width // 2]
        lines_ref[2 * place + 1 : 2 * place + 2] = value[:, width // 2 :]

    def loaded(place):
        halves = (lines_ref[2 * place : 2 * place + 1], lines_ref[2 * place + 1 : 2 * place + 2])
        return jnp.concatenate(halves, axis=1)

    copies = []

    def send(group):
        start, end = SENT[group]
        rows = pl.ds(start, end - start)
        for i in range(out_ref.shape[0]):
            copies.append(pltpu.make_async_copy(lines_ref.at[rows], out_ref.at[i, rows], sem.at[group, i]))
            copies[-1].start()

    store(0, pick(0, 1)[0])
    indices = lax.broadcasted_iota(jnp.int32, (1, width), 1)
    for number in range(ROUNDS):
        count = 1 << number
        first = indices < words_ref[count : count + 1]
        for right in range(count):
            *found, same = pick(count + right, right + 1)
            for left, value in enumerate(found):
                store(place_of(number, left, right), value)
            place = place_of(number, right, right)
            store(place, jnp.where(first, loaded(place), same) if right % 2 else same)
            if number == 3 and right == 6:
                send(0)
    send(1)
    for copy in copies:
        copy.wait()


def place_of(number, left, right):
    count = 1 << number
    start = (0, 2, 4, 12)[number] if number else 1
    if left == right:
        return start + count * (count - 1) // 2 + left // 2
    return start + right * (right - 1) // 2 + left


def table_of(words_ref, number):
    count = 1 << number
    return one_hot(words_ref[count : count + 1]).astype(BF16)


def angles_kernel(words_ref, part_ref, out_ref, sum_ref, lines_ref, moved_ref, state_ref):
    width = words_ref.shape[1]
    sum_ref[...] = jnp.sum(part_ref[...], axis=0)
    lines_ref[LINES:] = jnp.zeros((lines_ref.shape[0] - LINES, width), F32)
    for half in range(2):
        columns = slice(half * width // 2, (half + 1) * width // 2)
        lines_ref[:LINES, columns] = sum_ref[pl.ds(half, LINES, 2), :]
    tables = [table_of(words_ref, number) for number in range(ROUNDS)]
    for number, table in enumerate(tables):
        moved_ref[number] = permuted(lines_ref[...], table)
    indices = lax.broadcasted_iota(jnp.int32, (1, width), 1)
    state_ref[...] = jnp.zeros_like(state_ref)
    diag, diag_2 = lines_ref[:1], moved_ref[0, :1]
    weights, weights_2 = [jnp.ones((1, width), F32)], [jnp.ones((1, width), F32)]
    for number in range(ROUNDS):
        count = 1 << number
        if number:
            for i, value in enumerate([diag] + weights):
                state_ref[i : i + 1] = value
            other = permuted(state_ref[...], tables[number])
            diag_2, *weights_2 = (other[i : i + 1] for i in range(1 + count))
        first = indices < words_ref[count : count + 1]
        cross = jnp.zeros((1, width), F32)
        for left in range(count):
            inner = jnp.zeros((1, width), F32)
            for right in range(count):
                place = place_of(number, min(left, right), max(left, right))
                line, moved = lines_ref[place : place + 1], moved_ref[number, place : place + 1]
                if left == right and number:
                    line = jnp.where(first, moved, line) if left % 2 else jnp.where(first, line, moved)
                inner += weights_2[right] * (line if left <= right else moved)
            cross += weights[left] * inner
        orient = jnp.where(first, 1.0, -1.0)
        cos, sin = angle(orient, diag, diag_2, cross)
        diag = cos * cos * diag + 2.0 * cos * sin * cross + sin * sin * diag_2
        weights = [cos * value for value in weights] + [sin * value for value in weights_2]
    for i, value in enumerate(weights):
        out_ref[i : i + 1] = value


def plan_kernel(plan_ref, *words_refs):
    width = plan_ref.shape[1]
    for step, words_ref in enumerate(words_refs):
        words = lax.broadcasted_iota(jnp.int32, (1, width), 1)
        for number in range(ROUNDS):
            partner = plan_ref[step * ROUNDS + number : step * ROUNDS + number + 1]
            known = jnp.concatenate([words] * (WORDS // words.shape[0]), axis=0).astype(F32).astype(BF16)
            moved = jnp.dot(known, one_hot(partner).astype(BF16), preferred_element_type=F32)
            words = jnp.concatenate([words, moved[: words.shape[0]].astype(jnp.int32)], axis=0)
        words_ref[...] = words


def sort_kernel(in_ref, out_ref, held_ref, ready_ref, in_sem, out_sem):
    owners = out_ref.shape[0]
    lines, rows = held_ref.shape[1], ready_ref.shape[2]
    reads = [
        pltpu.make_async_copy(in_ref.at[pl.ds(i * lines, lines)], held_ref.at[i], in_sem.at[i]) for i in range(CHUNKS)
    ]
    writes = [
        pltpu.make_async_copy(ready_ref.at[i], out_ref.at[:, pl.ds(i * rows, rows)], out_sem.at[i])
        for i in range(CHUNKS)
    ]
    for read in reads:
        read.start()
    for i in range(CHUNKS):
        reads[i].wait()
        for j in range(2 * owners):
            half = j % 2 * 128
            ready_ref[i, j // 2, :, half : half + 128] = held_ref[i, pl.ds(j, rows, 2 * owners), :]
        writes[i].start()
    for write in writes:
        write.wait()


def unsort_kernel(in_ref, out_ref, ready_ref, out_sem):
    owners = in_ref.shape[0]
    lines = ready_ref.shape[1]
    rows = lines // (2 * owners)
    writes = [
        pltpu.make_async_copy(ready_ref.at[i], out_ref.at[pl.ds(i * lines, lines)], out_sem.at[i])
        for i in range(CHUNKS)
    ]
    for i in range(CHUNKS):
        for j in range(2 * owners):
            half = j % 2 * 128
            ready_ref[i, pl.ds(j, rows, 2 * owners), :] = in_ref[
                j // 2, i * rows : i * rows + rows, half : half + 128
            ]
        writes[i].start()
    for write in writes:
        write.wait()


def sorted_rows_of(lines, shape):
    owners, rows, across = shape
    return pl.pallas_call(
        sort_kernel,
        out_shape=pltpu.HBM(shape, F32),
        in_specs=[pl.BlockSpec(memory_space=pltpu.HBM)],
        out_specs=pl.BlockSpec(memory_space=pltpu.HBM),
        scratch_shapes=[
            pltpu.VMEM((CHUNKS, lines.shape[0] // CHUNKS, lines.shape[1]), F32),
            pltpu.VMEM((CHUNKS, owners, rows // CHUNKS, across), F32),
            pltpu.SemaphoreType.DMA((CHUNKS,)),
            pltpu.SemaphoreType.DMA((CHUNKS,)),
        ],
        compiler_params=pltpu.CompilerParams(vmem_limit_bytes=VMEM_BYTES),
    )(pltpu.with_memory_space_constraint(lines, pltpu.HBM))


def lines_from(value, shape):
    return pl.pallas_call(
        unsort_kernel,
        out_shape=pltpu.HBM(shape, F32),
        out_specs=pl.BlockSpec(memory_space=pltpu.HBM),
        scratch_shapes=[
            pltpu.VMEM((CHUNKS, shape[0] // CHUNKS, shape[1]), F32),
            pltpu.SemaphoreType.DMA((CHUNKS,)),
        ],
        compiler_params=pltpu.CompilerParams(vmem_limit_bytes=VMEM_BYTES),
    )(value)


def rotated(words_ref, weights_ref, x_ref, columns):
    line = lax.broadcasted_iota(jnp.int32, (x_ref.shape[1], columns.stop - columns.start), 0)
    rotation = jnp.zeros(line.shape, F32)
    for i in range(WORDS):
        rotation += jnp.where(line == words_ref[i : i + 1, columns], weights_ref[i : i + 1, columns], 0.0)
    return product(x_ref[...], rotation, 1)


def first_kernel(words_ref, x_ref, out_ref, moved_ref, lines_ref, sem):
    write_lines(x_ref[...], words_ref, out_ref, moved_ref, lines_ref, sem)


def top_kernel(words_ref, weights_ref, x_ref, top_ref):
    top_ref[...] = rotated(words_ref, weights_ref, x_ref, slice(0, top_ref.shape[1]))


def bottom_kernel(words_ref, weights_ref, x_ref, top_ref, y_ref):
    width = top_ref.shape[1]
    y_ref[:, :width] = top_ref[...]
    y_ref[:, width:] = rotated(words_ref, weights_ref, x_ref, slice(width, 2 * width))


def joined_kernel(
    words_ref, weights_ref, x_ref, top_ref, next_words_ref, out_ref, y_ref, moved_ref, lines_ref, sem
):
    bottom_kernel(words_ref, weights_ref, x_ref, top_ref, y_ref)
    write_lines(y_ref[...], next_words_ref, out_ref, moved_ref, lines_ref, sem)


def call(kernel, outs, *args, scratch=()):
    shapes = [jax.ShapeDtypeStruct(shape, dtype) for shape, dtype in outs]
    single = len(shapes) == 1
    return pl.pallas_call(
        kernel,
        out_shape=shapes[0] if single else shapes,
        scratch_shapes=[pltpu.VMEM(shape, F32) for shape in scratch],
        compiler_params=pltpu.CompilerParams(vmem_limit_bytes=VMEM_BYTES),
    )(*args)


def call_with_lines(kernel, sent, outs, *args):
    across = sent[1] * sent[2] // LINES
    return pl.pallas_call(
        kernel,
        out_shape=[pltpu.HBM(sent, F32)] + [jax.ShapeDtypeStruct(shape, F32) for shape in outs],
        out_specs=[pl.BlockSpec(memory_space=pltpu.HBM)] + [pl.BlockSpec(memory_space=pltpu.VMEM) for _ in outs],
        scratch_shapes=[
            pltpu.VMEM((WORDS // 2, across, across), F32),
            pltpu.VMEM(sent[1:], F32),
            pltpu.SemaphoreType.DMA((len(SENT), sent[0])),
        ],
        compiler_params=pltpu.CompilerParams(vmem_limit_bytes=VMEM_BYTES),
    )(*args)


def exchanged(value, axis):
    return lax.all_to_all(value, axis, split_axis=0, concat_axis=0, tiled=True)


def passed_along(block, axis, distance):
    devices = range(lax.axis_size(axis))
    route = [((i - distance) % len(devices), i) for i in devices]
    return lax.ppermute(block, axis, route)


def body(matrix, plan):
    rows, owners, halves, width = matrix.shape
    peers = lax.axis_size(SUMMED)
    across = halves * width
    flat = ((rows * owners, across), F32)
    half = ((rows * owners, width), F32)
    sorted_rows = (owners, rows, across)
    sent = (peers, 2 * LINES, across // 2)
    weights_shape = ((WORDS, across), F32)
    scratch = [sent[1:], (48, across), (ROUNDS, 48, across), (16, across)]
    lines = matrix.reshape(rows * owners * halves, width)
    x = exchanged(sorted_rows_of(lines, sorted_rows), OWNERS).reshape(flat[0])
    words_shape = ((WORDS, across), jnp.int32)
    words = call(plan_kernel, [words_shape] * STEPS, plan.reshape(-1, across))
    part = call_with_lines(first_kernel, sent, [], words[0], x)[0]
    for step in range(STEPS):
        x_before = passed_along(x, "cols", 1)
        part = exchanged(part, SUMMED)
        weights = call(angles_kernel, [weights_shape], words[step], part, scratch=scratch)
        weights_before = passed_along(weights, "cols", 1)
        top = call(top_kernel, [half], words[step], weights, x)
        args = (words[step], weights_before, x_before, top)
        if step + 1 < STEPS:
            part, x = call_with_lines(joined_kernel, sent, [flat[0]], *args, words[step + 1])
        else:
            x = call(bottom_kernel, [flat], *args)
    x = exchanged(x.reshape(sorted_rows), OWNERS)
    return lines_from(x, lines.shape).reshape(matrix.shape)


def solution(mesh):
    split = Mesh(mesh.devices.reshape(4, 8, 2, mesh.shape["cols"]), ("x", "z", "yh", "cols"))
    in_specs = (P(ROWS, "cols", None, None), P())
    out_specs = P(ROWS, "cols", None, None)
    return jax.shard_map(body, mesh=split, in_specs=in_specs, out_specs=out_specs, check_vma=False)
```
